32 devices in a mesh: dp: 2 (over x), cy: 4 (over z), cx: 4 (over y, core).
Axes of the slice: x: 2, y: 2, z: 4, core: 2. Of those that a mesh axis runs over, the one named last changes fastest.
Arguments:
- q: bfloat16 [8192, 32, 128], P(('dp', 'cy', 'cx')), parts along dimension 0
- k: bfloat16 [8192, 8, 128], P(('dp', 'cy', 'cx')), parts along dimension 0
- v: bfloat16 [8192, 8, 128], P(('dp', 'cy', 'cx')), parts along dimension 0
Outputs:
- output: bfloat16 [8192, 32, 128], P(('dp', 'cy', 'cx')), parts along dimension 0
There are 2 independent parts. The reference program is written for one: setup_inputs(seed, part) draws one part's arguments, and reference() takes and returns one part's arrays. A program takes and returns all parts, laid end to end along the dimension named above; each array names one.
All inputs are finite; a program needn't handle non-finite values.
Results may differ from the reference program's by a relative error of at most 0.00303333.
Values are sent between devices in bfloat16 or wider.
A program may use at most 1 GiB of HBM per device.

```python
import jax
import jax.numpy as jnp
from jax import lax

SEQ = 4096
NDEV = 16
HEADS = 32
KV_HEADS = 8
HEAD_DIM = 128

SPAN = SEQ // (2 * NDEV)
NEG = -1.0e30


def positions():
    i = jnp.arange(SEQ)
    blk = i // (2 * SPAN)
    j = i % (2 * SPAN)
    return jnp.where(j < SPAN, blk * SPAN + j, (2 * NDEV - 1 - blk) * SPAN + j - SPAN)


def setup_inputs(seed: int = 0, part: int = 0) -> dict:
    key = jax.random.fold_in(jax.random.key(seed), part)
    kq, kk, kv, ko = jax.random.split(key, 4)
    q = jax.random.normal(kq, (SEQ, HEADS, HEAD_DIM), jnp.float32)
    k = jax.random.normal(kk, (SEQ, KV_HEADS, HEAD_DIM), jnp.float32)
    off = jax.random.normal(ko, (2 * NDEV, 1, KV_HEADS, HEAD_DIM), jnp.float32)
    v = 0.5 * jax.random.normal(kv, (2 * NDEV, SPAN, KV_HEADS, HEAD_DIM), jnp.float32) + off
    v = v.reshape(SEQ, KV_HEADS, HEAD_DIM)
    return {'q': q.astype(jnp.bfloat16), 'k': k.astype(jnp.bfloat16), 'v': v.astype(jnp.bfloat16)}


def reference(q, k, v):
    rep = HEADS // KV_HEADS
    scale = HEAD_DIM ** -0.5
    pos = positions().reshape(2 * NDEV, SPAN)
    qc = q.reshape(2 * NDEV, SPAN, KV_HEADS, rep, HEAD_DIM)
    kc = k.reshape(2 * NDEV, SPAN, KV_HEADS, HEAD_DIM)
    vc = v.reshape(2 * NDEV, SPAN, KV_HEADS, HEAD_DIM)

    def one_query_span(xs):
        qb, pq = xs
        qf = qb.astype(jnp.float32)

        def step(carry, ys):
            m, l, acc = carry
            kb, vb, pk = ys
            s = jnp.einsum('qgrd,kgd->grqk', qf, kb.astype(jnp.float32)) * scale
            mask = pk[None, :] <= pq[:, None]
            s = jnp.where(mask, s, NEG)
            mn = jnp.maximum(m, jnp.max(s, axis=-1))
            p = jnp.where(mask, jnp.exp(s - mn[..., None]), 0.0)
            alpha = jnp.exp(m - mn)
            l = alpha * l + jnp.sum(p, axis=-1)
            pv = jnp.einsum('grqk,kgd->grqd', p.astype(jnp.bfloat16).astype(jnp.float32), vb.astype(jnp.float32))
            acc = alpha[..., None] * acc + pv
            return (mn, l, acc), None

        init = (jnp.full((KV_HEADS, rep, SPAN), NEG, jnp.float32),
                jnp.zeros((KV_HEADS, rep, SPAN), jnp.float32),
                jnp.zeros((KV_HEADS, rep, SPAN, HEAD_DIM), jnp.float32))
        (m, l, acc), _ = lax.scan(step, init, (kc, vc, pos))
        o = (acc / l[..., None]).astype(jnp.bfloat16)
        return o.transpose(2, 0, 1, 3).reshape(SPAN, HEADS, HEAD_DIM)

    out = lax.map(one_query_span, (qc, pos))
    return out.reshape(SEQ, HEADS, HEAD_DIM)
```

```python
import functools

import jax
import jax.numpy as jnp
from jax import lax
from jax.experimental import pallas as pl
from jax.experimental.pallas import tpu as pltpu
from jax.sharding import PartitionSpec as P

MESH = pl.DeviceIdType.MESH
NEG = -1.0e30
LOG2E = 1.4426950408889634
B = 512
S = 128
HD = 128

PUMP = ((1, 6, 2, 5, 3, 4), (2, 0, 5, 3, 4), (3, 1, 4, 0), (2, 1, 0))
STEPS = (
    (8 + 0, 8 + 1, 8 + 6, 8 + 2, 8 + 5, 8 + 3, 8 + 4),
    (8 + 1, 8 + 0, 0, 8 + 2, 8 + 5, 8 + 3, 8 + 4),
    (8 + 2, 8 + 1, 1, 8 + 3, 8 + 4, 8 + 0, 0),
    (8 + 3, 8 + 2, 2, 8 + 1, 1, 8 + 0, 0),
)
PRE = ((0, 4, 4, 0), (6, 7, 8, 3))
TARGET = (
    ((0, 1, 2, 3, 4, 5, 6), (4, 4, 5, 5, 5, 6, 6), (6, 6, 8, 8, 8, 8, 8), (0, 1, 1, 2, 2, 3, 3)),
    ((6, 7, 8, 9, 10, 11, 12), (7, 8, 8, 9, 9, 9, 10), (8, 8, 8, 8, 8, 8, 8), (3, 4, 4, 5, 5, 6, 6)),
)


def pick(z, values):
    out = jnp.int32(values[0])
    for i in range(1, len(values)):
        out = jnp.where(z == i, jnp.int32(values[i]), out)
    return out


def packed(seq):
    word = 0
    for i, x in enumerate(seq):
        word |= x << (4 * i)
    return word


def nibble(word, i):
    return lax.shift_right_logical(word, 4 * i) & 15


def kernel(q_ref, kv_ref, o_ref, qb, kvb, ob, mb, lb, ab,
           kv_s, kv_r, q_s, q_r, z_s, z_r, f_s, o_s, o_r, loc, oloc):
    dp = lax.axis_index("dp")
    z = lax.axis_index("cy")
    cx = lax.axis_index("cx")
    c = (HD ** -0.5) * LOG2E
    partners = (None, cx + 1 - 2 * (cx % 2), (cx + 2) % 4, 3 - cx)
    has_dn = z > 0
    has_up = z < 3

    def span_at(half, who):
        return (who if half == 0 else 3 - who) * S

    def blk(half):
        return z if half == 0 else 7 - z

    def kv_piece(h, half, who):
        return kvb.at[h, blk(half), :, pl.ds(span_at(half, who), S)]

    def kv_send(h, half, d):
        t = partners[d]
        return pltpu.make_async_remote_copy(
            kv_ref.at[2 * t + h, :, pl.ds(half * S, S)], kv_piece(h, half, cx),
            kv_s.at[h, half, d - 1], kv_r.at[h, half, d - 1],
            device_id=(dp, z, t), device_id_type=MESH)

    def kv_recv(h, half, d):
        ref = kv_piece(h, half, partners[d])
        return pltpu.make_async_remote_copy(
            ref, ref, kv_s.at[h, half, d - 1], kv_r.at[h, half, d - 1],
            device_id=(dp, z, partners[d]), device_id_type=MESH)

    def q_piece(h, half, who):
        return qb.at[h, :, pl.ds(half * B + span_at(half, who), S)]

    def q_send(h, half, d):
        t = partners[d]
        return pltpu.make_async_remote_copy(
            q_ref.at[pl.ds(8 * t + 4 * h, 4), pl.ds(half * S, S)], q_piece(h, half, cx),
            q_s.at[h, half, d - 1], q_r.at[h, half, d - 1],
            device_id=(dp, z, t), device_id_type=MESH)

    def q_recv(h, half, d):
        ref = q_piece(h, half, partners[d])
        return pltpu.make_async_remote_copy(
            ref, ref, q_s.at[h, half, d - 1], q_r.at[h, half, d - 1],
            device_id=(dp, z, partners[d]), device_id_type=MESH)

    def o_send(h, half, d):
        t = partners[d]
        return pltpu.make_async_remote_copy(
            ob.at[h, :, pl.ds(half * B + span_at(half, t), S)],
            o_ref.at[pl.ds(8 * cx + 4 * h, 4), pl.ds(half * S, S)],
            o_s.at[h, half, d - 1], o_r.at[h, half, d - 1],
            device_id=(dp, z, t), device_id_type=MESH)

    def o_recv(h, half, d):
        t = partners[d]
        ref = o_ref.at[pl.ds(8 * t + 4 * h, 4), pl.ds(half * S, S)]
        return pltpu.make_async_remote_copy(
            ref, ref, o_s.at[h, half, d - 1], o_r.at[h, half, d - 1],
            device_id=(dp, z, t), device_id_type=MESH)

    def z_own(h, half, d, way):
        if d == 0:
            src = kv_ref.at[2 * cx + h, :, pl.ds(half * S, S)]
            who = cx
        else:
            src = kv_piece(h, half, partners[d])
            who = partners[d]
        return pltpu.make_async_remote_copy(
            src, kv_piece(h, half, who), z_s.at[h, half, d, way], z_r.at[h, blk(half)],
            device_id=(dp, z + 1 if way == 0 else z - 1, cx), device_id_type=MESH)

    def z_fwd(h, b, way):
        return pltpu.make_async_remote_copy(
            kvb.at[h, b], kvb.at[h, b], f_s.at[h, b], z_r.at[h, b],
            device_id=(dp, z + 1 if way == 0 else z - 1, cx), device_id_type=MESH)

    barrier = pltpu.get_barrier_semaphore()
    for d in (1, 2, 3):
        pl.semaphore_signal(barrier, inc=1, device_id=(dp, z, partners[d]), device_id_type=MESH)

    @pl.when(has_dn)
    def _():
        pl.semaphore_signal(barrier, inc=1, device_id=(dp, z - 1, cx), device_id_type=MESH)

    @pl.when(has_up)
    def _():
        pl.semaphore_signal(barrier, inc=1, device_id=(dp, z + 1, cx), device_id_type=MESH)

    pl.semaphore_wait(barrier, 3 + jnp.where(has_dn, 1, 0) + jnp.where(has_up, 1, 0))

    def z_start(h, half, d):
        if half == 0:
            @pl.when(has_up)
            def _():
                z_own(h, half, d, 0).start()

        @pl.when(has_dn)
        def _():
            z_own(h, half, d, 1).start()

    def own_kv(h, half):
        return pltpu.make_async_copy(
            kv_ref.at[2 * cx + h, :, pl.ds(half * S, S)], kv_piece(h, half, cx), loc.at[0, h, half])

    def own_q(h, half):
        return pltpu.make_async_copy(
            q_ref.at[pl.ds(8 * cx + 4 * h, 4), pl.ds(half * S, S)], q_piece(h, half, cx), loc.at[1, h, half])

    for h in (0, 1):
        for half in (0, 1):
            for d in (2, 3, 1):
                kv_send(h, half, d).start()
            if h == 0:
                z_start(h, half, 0)
    for h in (0, 1):
        for half in (0, 1):
            for d in (2, 3, 1):
                q_send(h, half, d).start()
    for h in (0, 1):
        for half in (0, 1):
            own_kv(h, half).start()
            own_q(h, half).start()

    def relay_own(h):
        for half in (0, 1):
            if h == 1:
                z_start(h, half, 0)
            for d in (1, 2, 3):
                kv_recv(h, half, d).wait_recv()
                z_start(h, half, d)

    order = pick(z, [packed(p) for p in PUMP])
    per_head = 6 - z

    def pump(i, _):
        h = i // per_head
        b = nibble(order, i % per_head)
        ref = kvb.at[h, b]
        pltpu.make_async_remote_copy(
            ref, ref, f_s.at[h, b], z_r.at[h, b], device_id=(dp, z, partners[1]), device_id_type=MESH).wait_recv()
        from_up = jnp.logical_and(b > z, b < 7 - z)

        @pl.when(jnp.logical_and(has_dn, from_up))
        def _():
            z_fwd(h, b, 1).start()

        @pl.when(jnp.logical_and(has_up, b < z))
        def _():
            z_fwd(h, b, 0).start()

        return 0

    def fwd_wait(i, _):
        h = i // per_head
        b = nibble(order, i % per_head)
        from_up = jnp.logical_and(b > z, b < 7 - z)
        go = jnp.logical_or(jnp.logical_and(has_dn, from_up), jnp.logical_and(has_up, b < z))

        @pl.when(go)
        def _():
            z_fwd(h, b, 1).wait_send()

        return 0

    def diag(h, half, _):
        b = jnp.where(half == 0, z, 7 - z)
        for t in range(2):
            nk = (t + 1) * 256
            kk = kvb[h, b, 0, :nk]
            vv = kvb[h, b, 1, :nk]
            row = lax.broadcasted_iota(jnp.int32, (256, nk), 0) + t * 256
            mask = lax.broadcasted_iota(jnp.int32, (256, nk), 1) <= row
            for qh in range(4):
                sl = (qh, pl.ds(half * B + t * 256, 256))
                s = lax.dot_general(qb[(h,) + sl], kk, (((1,), (1,)), ((), ())), preferred_element_type=jnp.float32)
                s = jnp.where(mask, s, NEG)
                m = jnp.broadcast_to(jnp.max(s, axis=1, keepdims=True), (256, HD))
                p = jnp.exp2((s - jnp.concatenate([m] * (nk // HD), axis=1)) * c)
                mb[sl] = m
                tot = p[:, :HD]
                for j in range(1, nk // HD):
                    tot = tot + p[:, j * HD:(j + 1) * HD]
                lb[sl] = tot
                ab[sl] = jnp.dot(p.astype(jnp.bfloat16), vv, preferred_element_type=jnp.float32)
        return 0

    def full(h, half, b):
        kk = kvb[h, b, 0]
        vv = kvb[h, b, 1]
        for qh in range(4):
            sl = (qh, pl.ds(half * B, B))
            s = lax.dot_general(qb[(h,) + sl], kk, (((1,), (1,)), ((), ())), preferred_element_type=jnp.float32)
            m_old = mb[sl]
            m_new = jnp.maximum(m_old, jnp.max(s, axis=1, keepdims=True))
            alpha = jnp.exp2((m_old - m_new) * c)
            mb[sl] = m_new
            p = jnp.exp2((s - jnp.concatenate([m_new] * 4, axis=1)) * c)
            tot = (p[:, :128] + p[:, 128:256]) + (p[:, 256:384] + p[:, 384:])
            lb[sl] = alpha * lb[sl] + tot
            ab[sl] = alpha * ab[sl] + jnp.dot(p.astype(jnp.bfloat16), vv, preferred_element_type=jnp.float32)

    def o_own(h, half):
        return pltpu.make_async_copy(
            ob.at[h, :, pl.ds(half * B + span_at(half, cx), S)],
            o_ref.at[pl.ds(8 * cx + 4 * h, 4), pl.ds(half * S, S)], oloc.at[h, half])

    steps = pick(z, [packed(p) for p in STEPS])
    done = jnp.int32(0)

    def pump_to(lo, hi):
        lax.fori_loop(lo, hi, pump, 0)

    relay_own(0)
    pre0 = pick(z, PRE[0])
    pump_to(0, pre0)
    relay_own(1)
    for h in (0, 1):
        for half in (0, 1):
            own_kv(h, half).wait()

    for h in (0, 1):
        pre = pick(z, PRE[h])
        if h == 1:
            pump_to(pick(z, [t[-1] for t in TARGET[0]]), pre)
        for half in (0, 1):
            own_q(h, half).wait()
            for d in (1, 2, 3):
                q_recv(h, half, d).wait_recv()
        lax.fori_loop(0, 2, functools.partial(diag, h), 0)
        target = pick(z, [packed(t) for t in TARGET[h]])

        def step(i, at):
            hi = nibble(target, i)
            pump_to(at, hi)
            code = nibble(steps, i)
            full(h, code // 8, code % 8)
            return hi

        lax.fori_loop(0, 7, step, pre)

        def fin(i, _):
            sl = (i // 2, pl.ds((i % 2) * B, B))
            ob[(h,) + sl] = (ab[sl] / jnp.sum(lb[sl], axis=1, keepdims=True)).astype(jnp.bfloat16)
            return 0

        lax.fori_loop(0, 8, fin, 0)
        for half in (0, 1):
            for d in (2, 3, 1):
                o_send(h, half, d).start()
            o_own(h, half).start()

    lax.fori_loop(0, 2 * per_head, fwd_wait, 0)
    for h in (0, 1):
        for half in (0, 1):
            o_own(h, half).wait()
            for d in (1, 2, 3):
                kv_send(h, half, d).wait_send()
                q_send(h, half, d).wait_send()
                o_send(h, half, d).wait_send()
                o_recv(h, half, d).wait_recv()
            for d in range(4):
                if half == 0:
                    @pl.when(has_up)
                    def _():
                        z_own(h, half, d, 0).wait_send()

                @pl.when(has_dn)
                def _():
                    z_own(h, half, d, 1).wait_send()


def solution(mesh):
    spec = P(("dp", "cy", "cx"))

    def local(q, k, v):
        qt = q.transpose(1, 0, 2)
        kvt = jnp.stack([k, v]).transpose(2, 0, 1, 3)
        dma = pltpu.SemaphoreType.DMA
        out = pl.pallas_call(
            kernel,
            out_shape=jax.ShapeDtypeStruct((32, 256, HD), jnp.bfloat16),
            in_specs=[pl.BlockSpec(memory_space=pl.ANY)] * 2,
            out_specs=pl.BlockSpec(memory_space=pl.ANY),
            scratch_shapes=[
                pltpu.VMEM((2, 4, 2 * B, HD), jnp.bfloat16),
                pltpu.VMEM((2, 8, 2, B, HD), jnp.bfloat16),
                pltpu.VMEM((2, 4, 2 * B, HD), jnp.bfloat16),
                pltpu.VMEM((4, 2 * B, HD), jnp.float32),
                pltpu.VMEM((4, 2 * B, HD), jnp.float32),
                pltpu.VMEM((4, 2 * B, HD), jnp.float32),
                dma((2, 2, 3)), dma((2, 2, 3)),
                dma((2, 2, 3)), dma((2, 2, 3)),
                dma((2, 2, 4, 2)), dma((2, 8)), dma((2, 8)),
                dma((2, 2, 3)), dma((2, 2, 3)),
                dma((2, 2, 2)), dma((2, 2)),
            ],
            compiler_params=pltpu.CompilerParams(
                collective_id=0, has_side_effects=True, vmem_limit_bytes=60 * 1024 * 1024),
        )(qt, kvt)
        return out.transpose(1, 0, 2)

    return jax.shard_map(local, mesh=mesh, in_specs=(spec, spec, spec), out_specs=spec, check_vma=False)
```

```python
import jax
import jax.numpy as jnp
from jax import lax
from jax.experimental import pallas as pl
from jax.experimental.pallas import tpu as pltpu
from jax.sharding import PartitionSpec as P

MESH = pl.DeviceIdType.MESH
NEG = -1.0e30
LOG2E = 1.4426950408889634
B = 512
S = 128
HD = 128

PUMP = (
    (1, 6, 2, 5, 3, 4),
    (2, 0, 5, 3, 4, 8 + 0, 8 + 7, 8 + 2, 8 + 5, 8 + 3, 8 + 4),
    (3, 1, 4, 0, 8 + 3, 8 + 1, 8 + 4, 8 + 6, 8 + 0, 8 + 7),
    (2, 1, 0, 8 + 2, 8 + 1, 8 + 0),
)
ARRIVE = (
    (12, 17, 23, 29, 34, 40),
    (12, 12.5, 17, 23, 29, 21, 25, 35, 40, 46, 51),
    (12, 12.5, 17, 18, 23, 23.5, 29, 29.5, 34, 40),
    (12, 18, 23, 29, 34, 40),
)
FULL, DIAG, FIN, OTHER = 0, 1, 2, 3
L0, M0, H0, G0, L1, M1, H1, G1, X = range(9)
RELAY, MOVE = (OTHER, 0, 0), (OTHER, 0, 1)


def seq(group, blocks, z=None, fin=False):
    out = []
    if z is not None:
        out.append((DIAG, group, 7 if group == X else z if group % 4 < 2 else 7 - z))
    out += [(FULL, group, b) for b in blocks]
    if fin:
        out.append((FIN, group, 0))
    return out


PROGRAM = (
    seq(L0, (), 0, True) + seq(H0, (0, 1), 0) + [RELAY] + seq(L1, (), 0, True) + seq(H0, (6,)) + [MOVE]
    + seq(H0, (2,)) + seq(M0, (), 0, True) + seq(H0, (5,)) + seq(G0, (0, 1, 6, 2, 5, 3), 0) + seq(H0, (3,))
    + seq(M1, (), 0, True) + seq(G0, (4,), None, True) + seq(H0, (4,), None, True),
    seq(L0, (0,), 1, True) + seq(H0, (1, 0, 2), 1) + [RELAY] + seq(H0, (5,)) + seq(L1, (), 1) + seq(H1, (1,), 1)
    + seq(L1, (0,), None, True) + seq(H1, (0,)) + seq(H0, (3,)) + seq(M0, (0,), 1, True)
    + seq(G0, (1, 0, 2, 5, 3, 4), 1, True) + seq(H0, (4,), None, True) + seq(M1, (0,), 1, True)
    + seq(X, (6, 1, 0), 1) + seq(G1, (1, 0, 2, 5), 1) + seq(H1, (2, 5)) + seq(X, (2, 5)) + seq(G1, (3,))
    + seq(H1, (3,)) + seq(X, (3,)) + seq(G1, (4,), None, True) + seq(X, (4,), None, True) + seq(H1, (4,), None, True),
    seq(L0, (1,), 2) + seq(H0, (2, 1, 3), 2) + [RELAY] + seq(L0, (0,), None, True) + seq(H0, (4, 0), None, True)
    + seq(L1, (), 2) + seq(H1, (2,), 2) + seq(M0, (1, 0), 2, True) + seq(H1, (3, 1)) + seq(L1, (1,))
    + seq(G0, (2, 1, 3, 4, 0), 2, True) + seq(H1, (4,)) + seq(M1, (1, 0), 2, True) + seq(L1, (0,), None, True)
    + seq(H1, (0,), None, True) + seq(G1, (2, 1, 3, 4, 0), 2, True) + seq(X, (5, 6, 2, 1, 3, 4, 0), 2, True),
    seq(L0, (2,), 3) + seq(H0, (3, 2), 3) + [RELAY] + seq(L0, (1,)) + seq(H0, (1,)) + seq(L1, (), 3)
    + seq(H1, (3,), 3) + seq(L0, (0,), None, True) + seq(H0, (0,), None, True) + seq(M0, (2, 1, 0), 3, True)
    + seq(G0, (3, 2, 1, 0), 3, True) + seq(L1, (2,)) + seq(H1, (2,)) + seq(M1, (2, 1), 3) + seq(L1, (1,))
    + seq(H1, (1,)) + seq(G1, (3, 2, 1), 3) + seq(M1, (0,), None, True) + seq(G1, (0,), None, True)
    + seq(L1, (0,), None, True) + seq(H1, (0,), None, True),
)


def arrivals_taken(z):
    queries = {M0: 21.6, G0: 27, M1: 33, G1: 38, X: 30} if z else {M0: 27, G0: 33, M1: 38}
    t, taken, out = 10.6, 0, []
    for op, g, b in PROGRAM[z]:
        if op == FULL and b not in (z, 7 - z):
            code = (8 if g >= 4 else 0) + b
            n = PUMP[z].index(code)
            taken = max(taken, n + 1)
            t = max(t, ARRIVE[z][n])
        elif op == FULL and b == 7 - z and g == X:
            pass
        elif op == DIAG:
            t = max(t, queries.get(g, 0))
            if g == X:
                n = PUMP[z].index(8 + 7)
                taken = max(taken, n + 1)
                t = max(t, ARRIVE[z][n])
        elif op == OTHER:
            t = max(t, 21.6 if b else 16)
        while taken < len(PUMP[z]) and ARRIVE[z][taken] <= t:
            taken += 1
        out.append(taken)
        t += (0.75, 0.6, 0.3, 0.2)[op]
    return out


def pick(z, values):
    out = jnp.int32(values[0])
    for i in range(1, len(values)):
        out = jnp.where(z == i, jnp.int32(values[i]), out)
    return out


def words(z, seqs, bits):
    per = 31 // bits
    n = max(len(q) for q in seqs)
    return [pick(z, [sum(x << (bits * i) for i, x in enumerate(q[w:w + per])) for q in seqs])
            for w in range(0, n, per)]


def entry(table, i, bits):
    per = 31 // bits
    word = table[0]
    for w in range(1, len(table)):
        word = jnp.where(i >= per * w, table[w], word)
    return lax.shift_right_logical(word, bits * (i % per)) & ((1 << bits) - 1)


def kernel(q_ref, k_ref, v_ref, o_ref, qb, kvb, ob, mb, lb, ab,
           kv_s, kv_r, q_s, q_r, z_s, z_r, f_s, o_s, o_r, x_s, x_r, xo_s, xo_r, loc, oloc):
    dp = lax.axis_index("dp")
    z = lax.axis_index("cy")
    cx = lax.axis_index("cx")
    c = (HD ** -0.5) * LOG2E
    partners = (cx, cx + 1 - 2 * (cx % 2), (cx + 2) % 4, 3 - cx)
    first, second = z == 0, z == 1
    has_dn, has_up = z > 0, z < 3
    has_x = jnp.logical_and(z >= 1, z <= 2)

    def span_at(half, who):
        return (who if half == 0 else 3 - who) * S

    def blk(half):
        return z if half == 0 else 7 - z

    def remote(src, dst, ssem, rsem, dev):
        return pltpu.make_async_remote_copy(src, dst, ssem, rsem, device_id=dev, device_id_type=MESH)

    def kv_piece(h, half, who):
        return kvb.at[h, blk(half), :, pl.ds(span_at(half, who), S)]

    def kv_send(h, half, d):
        t = partners[d]
        for ref, n in ((k_ref, 0), (v_ref, 1)):
            remote(ref.at[2 * t + h, pl.ds(half * S, S)], kvb.at[h, blk(half), n, pl.ds(span_at(half, cx), S)],
                   kv_s.at[h, half, d - 1], kv_r.at[h, half, d - 1], (dp, z, t)).start()

    def kv_both(h, half, d):
        ref = kv_piece(h, half, partners[d])
        return remote(ref, ref, kv_s.at[h, half, d - 1], kv_r.at[h, half, d - 1], (dp, z, partners[d]))

    def rows4(ref, h, half, who):
        at = jnp.where(half == 0, who % 2, 1 - who % 2) * S
        return ref.at[pl.ds(((h * 2 + half) * 2 + who // 2) * 4, 4), pl.ds(at, S)]

    def q_piece(h, half, who):
        return rows4(qb, h, half, who)

    def q_send(h, half, d):
        t = partners[d]
        return remote(q_ref.at[pl.ds(8 * t + 4 * h, 4), pl.ds(half * S, S)], q_piece(h, half, cx),
                      q_s.at[h, half, d - 1], q_r.at[h, half, d - 1], (dp, z, t))

    def q_both(h, half, d):
        ref = q_piece(h, half, partners[d])
        return remote(ref, ref, q_s.at[h, half, d - 1], q_r.at[h, half, d - 1], (dp, z, partners[d]))

    def o_send(h, half, d):
        t = partners[d]
        return remote(rows4(ob, h, half, t),
                      o_ref.at[pl.ds(8 * cx + 4 * h, 4), pl.ds(half * S, S)],
                      o_s.at[h, half, d - 1], o_r.at[h, half, d - 1], (dp, z, t))

    def o_recv(h, half, d):
        t = partners[d]
        ref = o_ref.at[pl.ds(8 * t + 4 * h, 4), pl.ds(half * S, S)]
        return remote(ref, ref, o_s.at[h, half, d - 1], o_r.at[h, half, d - 1], (dp, z, t))

    def x_send(n):
        for y in (0, 1):
            remote(qb.at[pl.ds((6 + y) * 4 + 2 * n, 2)], qb.at[pl.ds(32 + 2 * y, 2)],
                   x_s.at[n], x_r.at[0], (dp, n + 1, cx)).start()

    def x_both(n):
        ref = qb.at[pl.ds(32, 4)]
        return remote(ref, ref, x_s.at[n], x_r.at[0], (dp, 0, cx))

    def xo_send(d):
        t = partners[d]
        return remote(ob.at[pl.ds(32 + 2 * (t // 2), 2), pl.ds((1 - t % 2) * S, S)],
                      o_ref.at[pl.ds(8 * cx + 2 + 2 * z, 2), pl.ds(S, S)],
                      xo_s.at[d], xo_r.at[z - 1, d], (dp, 0, t))

    def xo_recv(n, d):
        ref = o_ref.at[pl.ds(8 * partners[d] + 4 + 2 * n, 2), pl.ds(S, S)]
        return remote(ref, ref, xo_s.at[d], xo_r.at[n, d], (dp, n + 1, partners[d]))

    def z_dev(way):
        return (dp, z + 1 if way == 0 else z - 1, cx)

    def z_own(h, half, d, way):
        b = blk(half)
        if d == 0:
            for ref, n in ((k_ref, 0), (v_ref, 1)):
                remote(ref.at[2 * cx + h, pl.ds(half * S, S)], kvb.at[h, b, n, pl.ds(span_at(half, cx), S)],
                       z_s.at[h, half, d, way], z_r.at[h, b], z_dev(way)).start()
        else:
            z_piece(h, half, d, way).start()

    def z_piece(h, half, d, way):
        ref = kv_piece(h, half, partners[d])
        return remote(ref, ref, z_s.at[h, half, d, way], z_r.at[h, blk(half)], z_dev(way))

    def z_cond(h, half, way):
        if way == 0:
            return has_up if half == 0 else (z < 2 if h == 1 else None)
        return has_dn if h == 0 else z > 1

    def z_each(h, half, d, do):
        for way in (0, 1):
            cond = z_cond(h, half, way)
            if cond is not None:
                @pl.when(cond)
                def _():
                    do(h, half, d, way)

    def own_kv(h, half):
        for ref, n in ((k_ref, 0), (v_ref, 1)):
            pltpu.make_async_copy(ref.at[2 * cx + h, pl.ds(half * S, S)],
                                  kvb.at[h, blk(half), n, pl.ds(span_at(half, cx), S)], loc.at[0, h, half]).start()

    def own_kv_wait(h, half):
        ref = kv_piece(h, half, cx)
        pltpu.make_async_copy(ref, ref, loc.at[0, h, half]).wait()

    def own_q(h, half):
        return pltpu.make_async_copy(
            q_ref.at[pl.ds(8 * cx + 4 * h, 4), pl.ds(half * S, S)], q_piece(h, half, cx), loc.at[1, h, half])

    barrier = pltpu.get_barrier_semaphore()
    for n in range(1, 16):
        other = (z * 4 + cx + n) % 16
        pl.semaphore_signal(barrier, inc=1, device_id=(dp, other // 4, other % 4), device_id_type=MESH)
    pl.semaphore_wait(barrier, 15)

    for h in (0, 1):
        for half in (0, 1):
            for d in (2, 3, 1):
                kv_send(h, half, d)
            if h == 0:
                z_each(h, half, 0, z_own)

    def send_q(h, half):
        for d in (2, 3, 1):
            q_send(h, half, d).start()

    @pl.when(first)
    def _():
        send_q(1, 1)

    send_q(0, 0)
    send_q(0, 1)
    send_q(1, 0)

    @pl.when(jnp.logical_not(first))
    def _():
        send_q(1, 1)

    for h in (0, 1):
        for half in (0, 1):
            own_kv(h, half)
            own_q(h, half).start()

    def relay_own(h):
        for half in (0, 1):
            if h == 1:
                z_each(h, half, 0, z_own)
            for d in (1, 2, 3):
                kv_both(h, half, d).wait_recv()
                z_each(h, half, d, z_own)
            own_kv_wait(h, half)

    order = words(z, PUMP, 4)

    def z_fwd(h, b, way):
        ref = kvb.at[h, b]
        return remote(ref, ref, f_s.at[h, b], z_r.at[h, b], z_dev(way))

    def fwd_ways(h, b):
        from_up = jnp.logical_and(b > z, b < 7 - z)
        down = jnp.logical_and(from_up, jnp.logical_or(z > 1, jnp.logical_and(second, h == 0)))
        up = jnp.logical_or(jnp.logical_and(has_up, b < z), jnp.logical_and(second, b == 7))
        return up, down

    def pump(i, _):
        code = entry(order, i, 4)
        h, b = code // 8, code % 8
        ref = kvb.at[h, b]
        remote(ref, ref, f_s.at[h, b], z_r.at[h, b], (dp, z, partners[1])).wait_recv()
        up, down = fwd_ways(h, b)

        @pl.when(down)
        def _():
            z_fwd(h, b, 1).start()

        @pl.when(up)
        def _():
            z_fwd(h, b, 0).start()

        return 0

    def fwd_wait(i, _):
        code = entry(order, i, 4)
        h, b = code // 8, code % 8
        up, down = fwd_ways(h, b)

        @pl.when(jnp.logical_or(up, down))
        def _():
            ref = kvb.at[h, b]
            remote(ref, ref, f_s.at[h, b], z_r.at[h, b], (dp, z, partners[1])).wait_send()

        return 0

    def chain(items, kk, vv):
        def scores(it):
            tile, nk, _ = it
            return lax.dot_general(qb[tile], kk[:nk], (((1,), (1,)), ((), ())), preferred_element_type=jnp.float32)

        def value(pend):
            tile, nk, p, alpha = pend
            pv = jnp.dot(p, vv[:nk], preferred_element_type=jnp.float32)
            ab[tile] = pv if alpha is None else alpha * ab[tile] + pv

        s = scores(items[0])
        pend = None
        for n, it in enumerate(items):
            nxt = scores(items[n + 1]) if n + 1 < len(items) else None
            tile, nk, mask = it
            if mask is not None:
                s = jnp.where(mask, s, NEG)
            m = jnp.max(s, axis=1, keepdims=True)
            if mask is None:
                old = mb[tile]
                m = jnp.maximum(old, m)
                alpha = jnp.exp2((old - m) * c)
            else:
                m = jnp.broadcast_to(m, (256, HD))
                alpha = None
            mb[tile] = m
            p = jnp.exp2((s - jnp.concatenate([m] * (nk // HD), axis=1)) * c)
            tot = p[:, :HD]
            for j in range(1, nk // HD):
                tot = tot + p[:, j * HD:(j + 1) * HD]
            lb[tile] = tot if alpha is None else alpha * lb[tile] + tot
            if pend is not None:
                value(pend)
            pend = (tile, nk, p.astype(jnp.bfloat16), alpha)
            s = nxt
        value(pend)

    def full(g, h, b):
        chain([(g * 4 + t, B, None) for t in range(4)], kvb.at[h, b, 0], kvb.at[h, b, 1])

    def diag(g, h, b, lower):
        items = []
        for t, low in enumerate(lower):
            nk = 512 if low else 256
            row = lax.broadcasted_iota(jnp.int32, (256, nk), 0) + (256 if low else 0)
            mask = lax.broadcasted_iota(jnp.int32, (256, nk), 1) <= row
            items.append((g * 4 + t, nk, mask))
        chain(items, kvb.at[h, b, 0], kvb.at[h, b, 1])

    def o_own(h, half):
        return pltpu.make_async_copy(
            rows4(ob, h, half, cx),
            o_ref.at[pl.ds(8 * cx + 4 * h, 4), pl.ds(half * S, S)], oloc.at[h, half])

    relay_own(0)
    count = [len(p) for p in PROGRAM]
    ops = words(z, [[op | g << 2 | b << 6 | n << 9 for (op, g, b), n in zip(p, arrivals_taken(i))]
                    for i, p in enumerate(PROGRAM)], 13)

    def run(i, at):
        code = entry(ops, i, 13)
        op, gc, b, upto = code % 4, (code // 4) % 16, (code // 64) % 8, code // 512
        h = jnp.where(gc < 4, 0, 1)
        half = (gc // 2) % 2
        other = gc % 2
        extra = gc == X
        y = jnp.where(other == 0, cx // 2, 1 - cx // 2)
        g = jnp.where(extra, 8, gc - other + y)
        lax.fori_loop(at, upto, pump, 0)

        @pl.when(op == FULL)
        def _():
            full(g, h, b)

        @pl.when(op == DIAG)
        def _():
            lower = jnp.where(half == 0, y == 1, y == 0)

            @pl.when(extra)
            def _():
                x_both(0).wait_recv()
                diag(8, 1, 7, (True, True, False, False))

            @pl.when(jnp.logical_not(extra))
            def _():
                @pl.when(other == 0)
                def _():
                    own_q(h, half).wait()
                    q_both(h, half, 1).wait_recv()

                @pl.when(other == 1)
                def _():
                    q_both(h, half, 2).wait_recv()
                    q_both(h, half, 3).wait_recv()

                @pl.when(lower)
                def _():
                    diag(g, h, b, (True,) * 4)

                @pl.when(jnp.logical_not(lower))
                def _():
                    diag(g, h, b, (False,) * 4)

        @pl.when(op == FIN)
        def _():
            for t in range(4):
                tile = g * 4 + t
                ob[tile] = (ab[tile] / jnp.sum(lb[tile], axis=1, keepdims=True)).astype(jnp.bfloat16)

            @pl.when(extra)
            def _():
                for d in (2, 3, 1, 0):
                    xo_send(d).start()

            @pl.when(jnp.logical_not(extra))
            def _():
                @pl.when(other == 0)
                def _():
                    o_send(h, half, 1).start()
                    o_own(h, half).start()

                @pl.when(other == 1)
                def _():
                    o_send(h, half, 2).start()
                    o_send(h, half, 3).start()

        @pl.when(op == OTHER)
        def _():
            @pl.when(b == 0)
            def _():
                relay_own(1)

            @pl.when(b == 1)
            def _():
                own_q(1, 1).wait()
                for d in (1, 2, 3):
                    q_both(1, 1, d).wait_recv()
                for n in (0, 1):
                    x_send(n)

        return upto

    lax.fori_loop(0, pick(z, count), run, jnp.int32(0))

    lax.fori_loop(0, pick(z, [len(p) for p in PUMP]), fwd_wait, 0)

    def z_wait(h, half, d, way):
        z_piece(h, half, d, way).wait_send()

    for h in (0, 1):
        for half in (0, 1):
            for d in (1, 2, 3):
                kv_both(h, half, d).wait_send()
                q_send(h, half, d).wait_send()
            for d in range(4):
                z_each(h, half, d, z_wait)

            def o_wait():
                o_own(h, half).wait()
                for d in (1, 2, 3):
                    o_send(h, half, d).wait_send()
                    o_recv(h, half, d).wait_recv()

            if (h, half) == (1, 1):
                pl.when(jnp.logical_not(first))(o_wait)
            else:
                o_wait()

    @pl.when(first)
    def _():
        for n in (0, 1):
            x_both(n).wait_send()
            for d in range(4):
                xo_recv(n, d).wait_recv()

    @pl.when(has_x)
    def _():
        for d in range(4):
            xo_send(d).wait_send()


def solution(mesh):
    spec = P(("dp", "cy", "cx"))

    def local(q, k, v):
        qt, kt, vt = (x.transpose(1, 0, 2) for x in (q, k, v))
        dma = pltpu.SemaphoreType.DMA
        out = pl.pallas_call(
            kernel,
            out_shape=jax.ShapeDtypeStruct((32, 256, HD), jnp.bfloat16),
            in_specs=[pl.BlockSpec(memory_space=pl.ANY)] * 3,
            out_specs=pl.BlockSpec(memory_space=pl.ANY),
            scratch_shapes=[
                pltpu.VMEM((36, 256, HD), jnp.bfloat16),
                pltpu.VMEM((2, 8, 2, B, HD), jnp.bfloat16),
                pltpu.VMEM((36, 256, HD), jnp.bfloat16),
                pltpu.VMEM((36, 256, HD), jnp.float32),
                pltpu.VMEM((36, 256, HD), jnp.float32),
                pltpu.VMEM((36, 256, HD), jnp.float32),
                dma((2, 2, 3)), dma((2, 2, 3)),
                dma((2, 2, 3)), dma((2, 2, 3)),
                dma((2, 2, 4, 2)), dma((2, 8)), dma((2, 8)),
                dma((2, 2, 3)), dma((2, 2, 3)),
                dma((2,)), dma((1,)), dma((4,)), dma((2, 4)),
                dma((2, 2, 2)), dma((2, 2)),
            ],
            compiler_params=pltpu.CompilerParams(
                collective_id=0, has_side_effects=True, vmem_limit_bytes=60 * 1024 * 1024),
        )(qt, kt, vt)
        return out.transpose(1, 0, 2)

    return jax.shard_map(local, mesh=mesh, in_specs=(spec, spec, spec), out_specs=spec, check_vma=False)
```

```python
import jax
import jax.numpy as jnp
from jax import lax
from jax.experimental import pallas as pl
from jax.experimental.pallas import tpu as pltpu
from jax.sharding import PartitionSpec as P

MESH = pl.DeviceIdType.MESH
NEG = -1.0e30
LOG2E = 1.4426950408889634
B = 512
S = 128
HD = 128

PUMP = (
    (1, 6, 2, 5, 3, 4),
    (2, 0, 5, 3, 4, 8 + 0, 8 + 7, 8 + 2, 8 + 5, 8 + 3, 8 + 4),
    (3, 1, 4, 0, 8 + 3, 8 + 1, 8 + 4, 8 + 6, 8 + 0, 8 + 7),
    (2, 1, 0, 8 + 2, 8 + 1, 8 + 0),
)
ARRIVE = (
    (12, 17, 23, 29, 34, 40),
    (12, 12.5, 17, 23, 29, 21, 25, 35, 40, 46, 51),
    (12, 12.5, 17, 18, 23, 23.5, 29, 29.5, 34, 40),
    (12, 18, 23, 29, 34, 40),
)
FULL, DIAG, FIN, OTHER = 0, 1, 2, 3
L0, M0, H0, G0, L1, M1, H1, G1, X = range(9)
RELAY, MOVE = (OTHER, 0, 0), (OTHER, 0, 1)


def seq(group, blocks, z=None, fin=False):
    out = []
    if z is not None:
        out.append((DIAG, group, 7 if group == X else z if group % 4 < 2 else 7 - z))
    out += [(FULL, group, b) for b in blocks]
    if fin:
        out.append((FIN, group, 0))
    return out


PROGRAM = (
    seq(L0, (), 0, True) + seq(H0, (0, 1), 0) + [RELAY] + seq(L1, (), 0, True) + seq(H0, (6,)) + [MOVE]
    + seq(H0, (2,)) + seq(M0, (), 0, True) + seq(H0, (5,)) + seq(G0, (0, 1, 6, 2, 5, 3), 0) + seq(H0, (3,))
    + seq(M1, (), 0, True) + seq(G0, (4,), None, True) + seq(H0, (4,), None, True),
    seq(L0, (0,), 1, True) + seq(H0, (1, 0, 2), 1) + [RELAY] + seq(H0, (5,)) + seq(L1, (), 1) + seq(H1, (1,), 1)
    + seq(L1, (0,), None, True) + seq(H1, (0,)) + seq(H0, (3,)) + seq(M0, (0,), 1, True)
    + seq(G0, (1, 0, 2, 5, 3, 4), 1, True) + seq(H0, (4,), None, True) + seq(M1, (0,), 1, True)
    + seq(X, (6, 1, 0), 1) + seq(G1, (1, 0, 2, 5), 1) + seq(H1, (2, 5)) + seq(X, (2, 5)) + seq(G1, (3,))
    + seq(H1, (3,)) + seq(X, (3,)) + seq(G1, (4,), None, True) + seq(X, (4,), None, True) + seq(H1, (4,), None, True),
    seq(L0, (1,), 2) + seq(H0, (2, 1, 3), 2) + seq(L0, (0,), None, True) + seq(H0, (4,)) + [RELAY] + seq(H0, (0,), None, True)
    + seq(L1, (), 2) + seq(H1, (2,), 2) + seq(M0, (1, 0), 2, True) + seq(H1, (3, 1)) + seq(L1, (1,))
    + seq(G0, (2, 1, 3, 4, 0), 2, True) + seq(H1, (4,)) + seq(M1, (1, 0), 2, True) + seq(L1, (0,), None, True)
    + seq(H1, (0,), None, True) + seq(G1, (2, 1, 3, 4, 0), 2, True) + seq(X, (5, 6, 2, 1, 3, 4, 0), 2, True),
    seq(L0, (2,), 3) + seq(H0, (3, 2), 3) + [RELAY] + seq(L0, (1,)) + seq(H0, (1,)) + seq(L1, (), 3)
    + seq(H1, (3,), 3) + seq(L0, (0,), None, True) + seq(H0, (0,), None, True) + seq(M0, (2, 1, 0), 3, True)
    + seq(G0, (3, 2, 1, 0), 3, True) + seq(L1, (2,)) + seq(H1, (2,)) + seq(M1, (2, 1), 3) + seq(L1, (1,))
    + seq(H1, (1,)) + seq(G1, (3, 2, 1), 3) + seq(M1, (0,), None, True) + seq(G1, (0,), None, True)
    + seq(L1, (0,), None, True) + seq(H1, (0,), None, True),
)


def arrivals_taken(z):
    queries = {M0: 21.6, G0: 27, M1: 33, G1: 38, X: 30} if z else {M0: 27, G0: 33, M1: 38}
    t, taken, out = 10.6, 0, []
    for op, g, b in PROGRAM[z]:
        if op == FULL and b not in (z, 7 - z):
            code = (8 if g >= 4 else 0) + b
            n = PUMP[z].index(code)
            taken = max(taken, n + 1)
            t = max(t, ARRIVE[z][n])
        elif op == FULL and b == 7 - z and g == X:
            pass
        elif op == DIAG:
            t = max(t, queries.get(g, 0))
            if g == X:
                n = PUMP[z].index(8 + 7)
                taken = max(taken, n + 1)
                t = max(t, ARRIVE[z][n])
        elif op == OTHER:
            t = max(t, 21.6 if b else 16)
        while taken < len(PUMP[z]) and ARRIVE[z][taken] <= t:
            taken += 1
        out.append(taken)
        t += (0.9, 0.8, 0.5, 0.2)[op]
    return out


def pick(z, values):
    out = jnp.int32(values[0])
    for i in range(1, len(values)):
        out = jnp.where(z == i, jnp.int32(values[i]), out)
    return out


def words(z, seqs, bits):
    per = 31 // bits
    n = max(len(q) for q in seqs)
    return [pick(z, [sum(x << (bits * i) for i, x in enumerate(q[w:w + per])) for q in seqs])
            for w in range(0, n, per)]


def entry(table, i, bits):
    per = 31 // bits
    word = table[0]
    for w in range(1, len(table)):
        word = jnp.where(i >= per * w, table[w], word)
    return lax.shift_right_logical(word, bits * (i % per)) & ((1 << bits) - 1)


def kernel(q_ref, k_ref, v_ref, o_ref, qb, kvb, ob, mb, lb, ab,
           kv_s, kv_r, q_s, q_r, z_s, z_r, f_s, o_s, o_r, x_s, x_r, xo_s, xo_r, loc, oloc):
    dp = lax.axis_index("dp")
    z = lax.axis_index("cy")
    cx = lax.axis_index("cx")
    c = (HD ** -0.5) * LOG2E
    partners = (cx, cx + 1 - 2 * (cx % 2), (cx + 2) % 4, 3 - cx)
    first, second = z == 0, z == 1
    has_dn, has_up = z > 0, z < 3
    has_x = jnp.logical_and(z >= 1, z <= 2)

    def span_at(half, who):
        return (who if half == 0 else 3 - who) * S

    def blk(half):
        return z if half == 0 else 7 - z

    def remote(src, dst, ssem, rsem, dev):
        return pltpu.make_async_remote_copy(src, dst, ssem, rsem, device_id=dev, device_id_type=MESH)

    def kv_piece(h, half, who):
        return kvb.at[h, blk(half), :, pl.ds(span_at(half, who), S)]

    def kv_send(h, half, d):
        t = partners[d]
        for ref, n in ((k_ref, 0), (v_ref, 1)):
            remote(ref.at[2 * t + h, pl.ds(half * S, S)], kvb.at[h, blk(half), n, pl.ds(span_at(half, cx), S)],
                   kv_s.at[h, half, d - 1], kv_r.at[h, half, d - 1], (dp, z, t)).start()

    def kv_both(h, half, d):
        ref = kv_piece(h, half, partners[d])
        return remote(ref, ref, kv_s.at[h, half, d - 1], kv_r.at[h, half, d - 1], (dp, z, partners[d]))

    def rows4(ref, h, half, who):
        at = jnp.where(half == 0, who % 2, 1 - who % 2) * S
        return ref.at[pl.ds(((h * 2 + half) * 2 + who // 2) * 4, 4), pl.ds(at, S)]

    def q_piece(h, half, who):
        return rows4(qb, h, half, who)

    def q_send(h, half, d):
        t = partners[d]
        return remote(q_ref.at[pl.ds(8 * t + 4 * h, 4), pl.ds(half * S, S)], q_piece(h, half, cx),
                      q_s.at[h, half, d - 1], q_r.at[h, half, d - 1], (dp, z, t))

    def q_both(h, half, d):
        ref = q_piece(h, half, partners[d])
        return remote(ref, ref, q_s.at[h, half, d - 1], q_r.at[h, half, d - 1], (dp, z, partners[d]))

    def o_send(h, half, d):
        t = partners[d]
        return remote(rows4(ob, h, half, t),
                      o_ref.at[pl.ds(8 * cx + 4 * h, 4), pl.ds(half * S, S)],
                      o_s.at[h, half, d - 1], o_r.at[h, half, d - 1], (dp, z, t))

    def o_recv(h, half, d):
        t = partners[d]
        ref = o_ref.at[pl.ds(8 * t + 4 * h, 4), pl.ds(half * S, S)]
        return remote(ref, ref, o_s.at[h, half, d - 1], o_r.at[h, half, d - 1], (dp, z, t))

    def x_send(n):
        for y in (0, 1):
            remote(qb.at[pl.ds((6 + y) * 4 + 2 * n, 2)], qb.at[pl.ds(32 + 2 * y, 2)],
                   x_s.at[n], x_r.at[0], (dp, n + 1, cx)).start()

    def x_both(n):
        ref = qb.at[pl.ds(32, 4)]
        return remote(ref, ref, x_s.at[n], x_r.at[0], (dp, 0, cx))

    def xo_send(d):
        t = partners[d]
        return remote(ob.at[pl.ds(32 + 2 * (t // 2), 2), pl.ds((1 - t % 2) * S, S)],
                      o_ref.at[pl.ds(8 * cx + 2 + 2 * z, 2), pl.ds(S, S)],
                      xo_s.at[d], xo_r.at[z - 1, d], (dp, 0, t))

    def xo_recv(n, d):
        ref = o_ref.at[pl.ds(8 * partners[d] + 4 + 2 * n, 2), pl.ds(S, S)]
        return remote(ref, ref, xo_s.at[d], xo_r.at[n, d], (dp, n + 1, partners[d]))

    def z_dev(way):
        return (dp, z + 1 if way == 0 else z - 1, cx)

    def z_own(h, half, d, way):
        b = blk(half)
        if d == 0:
            for ref, n in ((k_ref, 0), (v_ref, 1)):
                remote(ref.at[2 * cx + h, pl.ds(half * S, S)], kvb.at[h, b, n, pl.ds(span_at(half, cx), S)],
                       z_s.at[h, half, d, way], z_r.at[h, b], z_dev(way)).start()
        else:
            z_piece(h, half, d, way).start()

    def z_piece(h, half, d, way):
        ref = kv_piece(h, half, partners[d])
        return remote(ref, ref, z_s.at[h, half, d, way], z_r.at[h, blk(half)], z_dev(way))

    def z_cond(h, half, way):
        if way == 0:
            return has_up if half == 0 else (z < 2 if h == 1 else None)
        return has_dn if h == 0 else z > 1

    def z_each(h, half, d, do):
        for way in (0, 1):
            cond = z_cond(h, half, way)
            if cond is not None:
                @pl.when(cond)
                def _():
                    do(h, half, d, way)

    def own_kv(h, half):
        for ref, n in ((k_ref, 0), (v_ref, 1)):
            pltpu.make_async_copy(ref.at[2 * cx + h, pl.ds(half * S, S)],
                                  kvb.at[h, blk(half), n, pl.ds(span_at(half, cx), S)], loc.at[0, h, half]).start()

    def own_kv_wait(h, half):
        ref = kv_piece(h, half, cx)
        pltpu.make_async_copy(ref, ref, loc.at[0, h, half]).wait()

    def own_q(h, half):
        return pltpu.make_async_copy(
            q_ref.at[pl.ds(8 * cx + 4 * h, 4), pl.ds(half * S, S)], q_piece(h, half, cx), loc.at[1, h, half])

    barrier = pltpu.get_barrier_semaphore()
    for n in range(1, 16):
        other = (z * 4 + cx + n) % 16
        pl.semaphore_signal(barrier, inc=1, device_id=(dp, other // 4, other % 4), device_id_type=MESH)
    pl.semaphore_wait(barrier, 15)

    for h in (0, 1):
        for half in (0, 1):
            for d in (2, 3, 1):
                kv_send(h, half, d)
            if h == 0:
                z_each(h, half, 0, z_own)

    def send_q(h, half):
        for d in (2, 3, 1):
            q_send(h, half, d).start()

    @pl.when(first)
    def _():
        send_q(1, 1)

    send_q(0, 0)
    send_q(0, 1)
    send_q(1, 0)

    @pl.when(jnp.logical_not(first))
    def _():
        send_q(1, 1)

    for h in (0, 1):
        for half in (0, 1):
            own_kv(h, half)
            own_q(h, half).start()

    def relay_own(h):
        for half in (0, 1):
            if h == 1:
                z_each(h, half, 0, z_own)
            for d in (1, 2, 3):
                kv_both(h, half, d).wait_recv()
                z_each(h, half, d, z_own)
            own_kv_wait(h, half)

    order = words(z, PUMP, 4)

    def z_fwd(h, b, way):
        ref = kvb.at[h, b]
        return remote(ref, ref, f_s.at[h, b], z_r.at[h, b], z_dev(way))

    def fwd_ways(h, b):
        from_up = jnp.logical_and(b > z, b < 7 - z)
        down = jnp.logical_and(from_up, jnp.logical_or(z > 1, jnp.logical_and(second, h == 0)))
        up = jnp.logical_or(jnp.logical_and(has_up, b < z), jnp.logical_and(second, b == 7))
        return up, down

    def pump(i, _):
        code = entry(order, i, 4)
        h, b = code // 8, code % 8
        ref = kvb.at[h, b]
        remote(ref, ref, f_s.at[h, b], z_r.at[h, b], (dp, z, partners[1])).wait_recv()
        up, down = fwd_ways(h, b)

        @pl.when(down)
        def _():
            z_fwd(h, b, 1).start()

        @pl.when(up)
        def _():
            z_fwd(h, b, 0).start()

        return 0

    def fwd_wait(i, _):
        code = entry(order, i, 4)
        h, b = code // 8, code % 8
        up, down = fwd_ways(h, b)

        @pl.when(jnp.logical_or(up, down))
        def _():
            ref = kvb.at[h, b]
            remote(ref, ref, f_s.at[h, b], z_r.at[h, b], (dp, z, partners[1])).wait_send()

        return 0

    def chain(items, kk, vv):
        def scores(it):
            tile, nk, _ = it
            return lax.dot_general(qb[tile], kk[:nk], (((1,), (1,)), ((), ())), preferred_element_type=jnp.float32)

        def value(pend):
            tile, nk, p, alpha = pend
            pv = jnp.dot(p, vv[:nk], preferred_element_type=jnp.float32)
            ab[tile] = pv if alpha is None else alpha * ab[tile] + pv

        s = scores(items[0])
        pend = None
        for n, it in enumerate(items):
            nxt = scores(items[n + 1]) if n + 1 < len(items) else None
            tile, nk, mask = it
            if mask is not None:
                s = jnp.where(mask, s, NEG)
            m = jnp.max(s, axis=1, keepdims=True)
            if mask is None:
                old = mb[tile]
                m = jnp.maximum(old, m)
                alpha = jnp.exp2((old - m) * c)
            else:
                m = jnp.broadcast_to(m, (256, HD))
                alpha = None
            mb[tile] = m
            p = jnp.exp2((s - jnp.concatenate([m] * (nk // HD), axis=1)) * c)
            tot = p[:, :HD]
            for j in range(1, nk // HD):
                tot = tot + p[:, j * HD:(j + 1) * HD]
            lb[tile] = tot if alpha is None else alpha * lb[tile] + tot
            if pend is not None:
                value(pend)
            pend = (tile, nk, p.astype(jnp.bfloat16), alpha)
            s = nxt
        value(pend)

    def full(g, h, b):
        chain([(g * 4 + t, B, None) for t in range(4)], kvb.at[h, b, 0], kvb.at[h, b, 1])

    def diag(g, h, b, lower):
        items = []
        for t, low in enumerate(lower):
            nk = 512 if low else 256
            row = lax.broadcasted_iota(jnp.int32, (256, nk), 0) + (256 if low else 0)
            mask = lax.broadcasted_iota(jnp.int32, (256, nk), 1) <= row
            items.append((g * 4 + t, nk, mask))
        chain(items, kvb.at[h, b, 0], kvb.at[h, b, 1])

    def o_own(h, half):
        return pltpu.make_async_copy(
            rows4(ob, h, half, cx),
            o_ref.at[pl.ds(8 * cx + 4 * h, 4), pl.ds(half * S, S)], oloc.at[h, half])

    relay_own(0)
    count = [len(p) for p in PROGRAM]
    ops = words(z, [[op | g << 2 | b << 6 | n << 9 for (op, g, b), n in zip(p, arrivals_taken(i))]
                    for i, p in enumerate(PROGRAM)], 13)

    def run(i, at):
        code = entry(ops, i, 13)
        op, gc, b, upto = code % 4, (code // 4) % 16, (code // 64) % 8, code // 512
        h = jnp.where(gc < 4, 0, 1)
        half = (gc // 2) % 2
        other = gc % 2
        extra = gc == X
        y = jnp.where(other == 0, cx // 2, 1 - cx // 2)
        g = jnp.where(extra, 8, gc - other + y)
        lax.fori_loop(at, upto, pump, 0)

        @pl.when(op == FULL)
        def _():
            full(g, h, b)

        @pl.when(op == DIAG)
        def _():
            lower = jnp.where(half == 0, y == 1, y == 0)

            @pl.when(extra)
            def _():
                x_both(0).wait_recv()
                diag(8, 1, 7, (True, True, False, False))

            @pl.when(jnp.logical_not(extra))
            def _():
                @pl.when(other == 0)
                def _():
                    own_q(h, half).wait()
                    q_both(h, half, 1).wait_recv()

                @pl.when(other == 1)
                def _():
                    q_both(h, half, 2).wait_recv()
                    q_both(h, half, 3).wait_recv()

                @pl.when(lower)
                def _():
                    diag(g, h, b, (True,) * 4)

                @pl.when(jnp.logical_not(lower))
                def _():
                    diag(g, h, b, (False,) * 4)

        @pl.when(op == FIN)
        def _():
            for t in range(4):
                tile = g * 4 + t
                ob[tile] = (ab[tile] / jnp.sum(lb[tile], axis=1, keepdims=True)).astype(jnp.bfloat16)

            @pl.when(extra)
            def _():
                for d in (2, 3, 1, 0):
                    xo_send(d).start()

            @pl.when(jnp.logical_not(extra))
            def _():
                @pl.when(other == 0)
                def _():
                    o_send(h, half, 1).start()
                    o_own(h, half).start()

                @pl.when(other == 1)
                def _():
                    o_send(h, half, 2).start()
                    o_send(h, half, 3).start()

        @pl.when(op == OTHER)
        def _():
            @pl.when(b == 0)
            def _():
                relay_own(1)

            @pl.when(b == 1)
            def _():
                own_q(1, 1).wait()
                for d in (1, 2, 3):
                    q_both(1, 1, d).wait_recv()
                for n in (0, 1):
                    x_send(n)

        return upto

    lax.fori_loop(0, pick(z, count), run, jnp.int32(0))

    lax.fori_loop(0, pick(z, [len(p) for p in PUMP]), fwd_wait, 0)

    def z_wait(h, half, d, way):
        z_piece(h, half, d, way).wait_send()

    for h in (0, 1):
        for half in (0, 1):
            for d in (1, 2, 3):
                kv_both(h, half, d).wait_send()
                q_send(h, half, d).wait_send()
            for d in range(4):
                z_each(h, half, d, z_wait)

            def o_wait():
                o_own(h, half).wait()
                for d in (1, 2, 3):
                    o_send(h, half, d).wait_send()
                    o_recv(h, half, d).wait_recv()

            if (h, half) == (1, 1):
                pl.when(jnp.logical_not(first))(o_wait)
            else:
                o_wait()

    @pl.when(first)
    def _():
        for n in (0, 1):
            x_both(n).wait_send()
            for d in range(4):
                xo_recv(n, d).wait_recv()

    @pl.when(has_x)
    def _():
        for d in range(4):
            xo_send(d).wait_send()


def solution(mesh):
    spec = P(("dp", "cy", "cx"))

    def local(q, k, v):
        qt, kt, vt = (x.transpose(1, 0, 2) for x in (q, k, v))
        dma = pltpu.SemaphoreType.DMA
        out = pl.pallas_call(
            kernel,
            out_shape=jax.ShapeDtypeStruct((32, 256, HD), jnp.bfloat16),
            in_specs=[pl.BlockSpec(memory_space=pl.ANY)] * 3,
            out_specs=pl.BlockSpec(memory_space=pl.ANY),
            scratch_shapes=[
                pltpu.VMEM((36, 256, HD), jnp.bfloat16),
                pltpu.VMEM((2, 8, 2, B, HD), jnp.bfloat16),
                pltpu.VMEM((36, 256, HD), jnp.bfloat16),
                pltpu.VMEM((36, 256, HD), jnp.float32),
                pltpu.VMEM((36, 256, HD), jnp.float32),
                pltpu.VMEM((36, 256, HD), jnp.float32),
                dma((2, 2, 3)), dma((2, 2, 3)),
                dma((2, 2, 3)), dma((2, 2, 3)),
                dma((2, 2, 4, 2)), dma((2, 8)), dma((2, 8)),
                dma((2, 2, 3)), dma((2, 2, 3)),
                dma((2,)), dma((1,)), dma((4,)), dma((2, 4)),
                dma((2, 2, 2)), dma((2, 2)),
            ],
            compiler_params=pltpu.CompilerParams(
                collective_id=0, has_side_effects=True, vmem_limit_bytes=60 * 1024 * 1024),
        )(qt, kt, vt)
        return out.transpose(1, 0, 2)

    return jax.shard_map(local, mesh=mesh, in_specs=(spec, spec, spec), out_specs=spec, check_vma=False)
```

```python
import jax
import jax.numpy as jnp
from jax import lax
from jax.experimental import pallas as pl
from jax.experimental.pallas import tpu as pltpu
from jax.sharding import PartitionSpec as P

MESH = pl.DeviceIdType.MESH
NEG = -1.0e30
LOG2E = 1.4426950408889634
B = 512
S = 128
HD = 128

PUMP = (
    (1, 6, 2, 5, 3, 4,),
    (0, 2, 5, 3, 8, 4, 10, 13, 15, 11, 12,),
    (1, 3, 4, 0, 11, 9, 12, 8, 14, 15,),
    (2, 1, 10, 0, 9, 8,),
)
FULL, DIAG, FIN, OTHER, PAIR, TRIO = range(6)
L0, M0, H0, G0, L1, M1, H1, G1, X = range(9)
PROGRAM = (
    ((1, 0, 0, 0), (2, 0, 0, 0), (1, 2, 7, 0), (0, 2, 1, 1), (0, 2, 0, 1), (3, 0, 0, 2), (1, 4, 0, 2),
     (2, 4, 0, 2), (0, 2, 6, 2), (3, 0, 1, 3), (3, 0, 2, 3), (0, 2, 2, 3), (1, 1, 0, 4), (2, 1, 0, 4),
     (0, 2, 5, 4), (1, 3, 7, 5), (0, 3, 1, 5), (0, 3, 2, 5), (4, 2, 3, 5), (0, 3, 5, 5), (0, 3, 6, 5),
     (4, 2, 4, 6), (0, 3, 0, 6), (2, 3, 0, 6), (2, 2, 0, 6), (1, 5, 0, 6), (2, 5, 0, 6),),
    ((1, 0, 1, 0), (1, 2, 6, 0), (0, 0, 0, 1), (2, 0, 0, 2), (0, 2, 0, 2), (0, 2, 2, 2), (0, 2, 1, 2),
     (3, 0, 0, 3), (1, 4, 1, 3), (1, 6, 6, 3), (0, 6, 1, 3), (0, 2, 5, 3), (1, 1, 1, 4), (0, 1, 0, 4),
     (2, 1, 0, 4), (0, 2, 3, 4), (3, 0, 2, 5), (0, 4, 0, 5), (2, 4, 0, 5), (0, 6, 0, 5), (1, 3, 6, 6),
     (0, 3, 0, 6), (0, 3, 2, 6), (0, 3, 3, 6), (4, 2, 4, 6), (0, 3, 5, 6), (1, 5, 1, 7), (0, 5, 0, 7),
     (2, 5, 0, 7), (0, 6, 2, 7), (0, 3, 1, 7), (2, 3, 0, 7), (2, 2, 0, 7), (0, 6, 5, 8), (1, 7, 6, 8),
     (0, 7, 0, 8), (3, 0, 3, 9), (0, 8, 0, 9), (0, 8, 2, 9), (0, 8, 5, 9), (5, 6, 3, 10), (1, 8, 7, 10),
     (0, 8, 1, 10), (0, 8, 6, 10), (0, 7, 2, 10), (5, 6, 4, 11), (2, 8, 0, 11), (2, 6, 0, 11), (0, 7, 5, 11),
     (0, 7, 1, 11), (2, 7, 0, 11),),
    ((1, 0, 2, 0), (1, 2, 5, 0), (0, 0, 1, 1), (0, 2, 1, 2), (0, 2, 3, 2), (0, 2, 2, 2), (3, 0, 0, 3),
     (1, 6, 5, 3), (0, 6, 2, 3), (0, 2, 4, 3), (1, 4, 2, 3), (0, 0, 0, 4), (2, 0, 0, 4), (0, 2, 0, 4),
     (1, 1, 2, 4), (0, 1, 0, 4), (0, 1, 1, 4), (0, 6, 3, 5), (0, 6, 1, 6), (2, 1, 0, 6), (2, 2, 0, 6),
     (0, 4, 1, 6), (1, 3, 5, 6), (0, 3, 0, 6), (0, 6, 4, 7), (0, 3, 1, 7), (0, 3, 3, 7), (1, 5, 2, 7),
     (0, 5, 1, 7), (0, 3, 4, 7), (0, 3, 2, 7), (0, 6, 0, 8), (2, 6, 0, 8), (4, 4, 0, 8), (2, 5, 0, 8),
     (1, 7, 5, 8), (0, 7, 0, 8), (0, 7, 1, 9), (0, 7, 3, 9), (0, 7, 4, 9), (0, 7, 2, 9), (2, 7, 0, 9),
     (2, 4, 0, 9), (2, 3, 0, 9), (3, 0, 3, 10), (0, 8, 0, 10), (0, 8, 1, 10), (0, 8, 3, 10), (0, 8, 4, 10),
     (0, 8, 6, 10), (1, 8, 7, 10), (0, 8, 2, 10), (0, 8, 5, 10), (2, 8, 0, 10),),
    ((1, 0, 3, 0), (1, 2, 4, 0), (0, 0, 2, 1), (0, 2, 2, 1), (0, 2, 3, 1), (3, 0, 0, 1), (1, 6, 4, 1),
     (0, 6, 3, 1), (1, 4, 3, 1), (0, 0, 1, 2), (0, 2, 1, 2), (1, 1, 3, 2), (0, 1, 1, 2), (0, 1, 2, 2),
     (0, 6, 2, 3), (0, 4, 2, 3), (1, 3, 4, 3), (0, 3, 1, 3), (0, 3, 2, 3), (0, 3, 3, 3), (4, 0, 0, 4),
     (2, 0, 0, 4), (4, 2, 0, 4), (2, 2, 0, 4), (2, 1, 0, 4), (2, 3, 0, 4), (1, 5, 3, 4), (0, 6, 1, 5),
     (4, 4, 1, 5), (1, 7, 4, 5), (0, 7, 1, 5), (0, 7, 2, 5), (0, 7, 3, 5), (0, 5, 2, 5), (4, 6, 0, 6),
     (2, 6, 0, 6), (2, 7, 0, 6), (4, 4, 0, 6), (2, 4, 0, 6), (2, 5, 0, 6),),
)


def pick(z, values):
    out = jnp.int32(values[0])
    for i in range(1, len(values)):
        out = jnp.where(z == i, jnp.int32(values[i]), out)
    return out


def words(z, seqs, bits):
    per = 31 // bits
    n = max(len(q) for q in seqs)
    return [pick(z, [sum(x << (bits * i) for i, x in enumerate(q[w:w + per])) for q in seqs])
            for w in range(0, n, per)]


def entry(table, i, bits):
    per = 31 // bits
    word = table[0]
    for w in range(1, len(table)):
        word = jnp.where(i >= per * w, table[w], word)
    return lax.shift_right_logical(word, bits * (i % per)) & ((1 << bits) - 1)


def kernel(q_in, k_in, v_in, o_ref, q_raw, k_raw, v_raw, q_ref, k_ref, v_ref, qb, kvb, ob, mb, lb, ab,
           kv_s, kv_r, q_s, q_r, z_s, z_r, f_s, o_s, o_r, x_s, x_r, xo_s, xo_r, loc, oloc):
    dp = lax.axis_index("dp")
    z = lax.axis_index("cy")
    cx = lax.axis_index("cx")
    c = (HD ** -0.5) * LOG2E
    partners = (cx, cx + 1 - 2 * (cx % 2), (cx + 2) % 4, 3 - cx)
    first, second = z == 0, z == 1
    has_dn, has_up = z > 0, z < 3
    has_x = jnp.logical_and(z >= 1, z <= 2)

    def span_at(half, who):
        return (who if half == 0 else 3 - who) * S

    def blk(half):
        return z if half == 0 else 7 - z

    def remote(src, dst, ssem, rsem, dev):
        return pltpu.make_async_remote_copy(src, dst, ssem, rsem, device_id=dev, device_id_type=MESH)

    def kv_piece(h, half, who):
        return kvb.at[h, blk(half), :, pl.ds(span_at(half, who), S)]

    def kv_send(h, half, d):
        t = partners[d]
        for ref, n in ((k_ref, 0), (v_ref, 1)):
            remote(ref.at[2 * t + h, pl.ds(half * S, S)], kvb.at[h, blk(half), n, pl.ds(span_at(half, cx), S)],
                   kv_s.at[h, half, d - 1], kv_r.at[h, half, d - 1], (dp, z, t)).start()

    def kv_both(h, half, d):
        ref = kv_piece(h, half, partners[d])
        return remote(ref, ref, kv_s.at[h, half, d - 1], kv_r.at[h, half, d - 1], (dp, z, partners[d]))

    def rows4(ref, h, half, who):
        at = jnp.where(half == 0, who % 2, 1 - who % 2) * S
        return ref.at[pl.ds(((h * 2 + half) * 2 + who // 2) * 4, 4), pl.ds(at, S)]

    def q_piece(h, half, who):
        return rows4(qb, h, half, who)

    def q_send(h, half, d):
        t = partners[d]
        return remote(q_ref.at[pl.ds(8 * t + 4 * h, 4), pl.ds(half * S, S)], q_piece(h, half, cx),
                      q_s.at[h, half, d - 1], q_r.at[h, half, d - 1], (dp, z, t))

    def q_both(h, half, d):
        ref = q_piece(h, half, partners[d])
        return remote(ref, ref, q_s.at[h, half, d - 1], q_r.at[h, half, d - 1], (dp, z, partners[d]))

    def o_send(h, half, d):
        t = partners[d]
        return remote(rows4(ob, h, half, t),
                      o_ref.at[pl.ds(8 * cx + 4 * h, 4), pl.ds(half * S, S)],
                      o_s.at[h, half, d - 1], o_r.at[h, half, d - 1], (dp, z, t))

    def o_recv(h, half, d):
        t = partners[d]
        ref = o_ref.at[pl.ds(8 * t + 4 * h, 4), pl.ds(half * S, S)]
        return remote(ref, ref, o_s.at[h, half, d - 1], o_r.at[h, half, d - 1], (dp, z, t))

    def x_send(n):
        for y in (0, 1):
            remote(qb.at[pl.ds((6 + y) * 4 + 2 * n, 2)], qb.at[pl.ds(32 + 2 * y, 2)],
                   x_s.at[n], x_r.at[0], (dp, n + 1, cx)).start()

    def x_both(n):
        ref = qb.at[pl.ds(32, 4)]
        return remote(ref, ref, x_s.at[n], x_r.at[0], (dp, 0, cx))

    def xo_send(d):
        t = partners[d]
        return remote(ob.at[pl.ds(32 + 2 * (t // 2), 2), pl.ds((1 - t % 2) * S, S)],
                      o_ref.at[pl.ds(8 * cx + 2 + 2 * z, 2), pl.ds(S, S)],
                      xo_s.at[d], xo_r.at[z - 1, d], (dp, 0, t))

    def xo_recv(n, d):
        ref = o_ref.at[pl.ds(8 * partners[d] + 4 + 2 * n, 2), pl.ds(S, S)]
        return remote(ref, ref, xo_s.at[d], xo_r.at[n, d], (dp, n + 1, partners[d]))

    def z_dev(way):
        return (dp, z + 1 if way == 0 else z - 1, cx)

    def z_own(h, half, d, way):
        b = blk(half)
        if d == 0:
            for ref, n in ((k_ref, 0), (v_ref, 1)):
                remote(ref.at[2 * cx + h, pl.ds(half * S, S)], kvb.at[h, b, n, pl.ds(span_at(half, cx), S)],
                       z_s.at[h, half, d, way], z_r.at[h, b], z_dev(way)).start()
        else:
            z_piece(h, half, d, way).start()

    def z_piece(h, half, d, way):
        ref = kv_piece(h, half, partners[d])
        return remote(ref, ref, z_s.at[h, half, d, way], z_r.at[h, blk(half)], z_dev(way))

    def z_cond(h, half, way):
        if way == 0:
            return has_up if half == 0 else None
        return has_dn if h == 0 else z > 1

    def z_each(h, half, d, do):
        for way in (0, 1):
            cond = z_cond(h, half, way)
            if cond is not None:
                @pl.when(cond)
                def _():
                    do(h, half, d, way)

    def own_kv(h, half):
        for ref, n in ((k_ref, 0), (v_ref, 1)):
            kvb[h, blk(half), n, pl.ds(span_at(half, cx), S)] = ref[2 * cx + h, half * S:(half + 1) * S]

    def own_q(h, half):
        at = (cx % 2 if half == 0 else 1 - cx % 2) * S
        for t in range(4):
            qb[((h * 2 + half) * 2 + cx // 2) * 4 + t, pl.ds(at, S)] = q_ref[8 * cx + 4 * h + t, half * S:(half + 1) * S]

    loads = [pltpu.make_async_copy(src, dst, loc.at[n])
             for n, (src, dst) in enumerate(((k_in, k_raw), (v_in, v_raw), (q_in, q_raw)))]
    for copy in loads:
        copy.start()

    barrier = pltpu.get_barrier_semaphore()
    for n in range(1, 16):
        other = (z * 4 + cx + n) % 16
        pl.semaphore_signal(barrier, inc=1, device_id=(dp, other // 4, other % 4), device_id_type=MESH)
    for copy, src, dst in zip(loads[:2], (k_raw, v_raw), (k_ref, v_ref)):
        copy.wait()
        dst[...] = jnp.swapaxes(src[...], 0, 1)
    pl.semaphore_wait(barrier, 15)

    for h in (0, 1):
        for half in (0, 1):
            for d in (2, 3, 1):
                kv_send(h, half, d)
            if h == 0:
                z_each(h, half, 0, z_own)

    for h in (0, 1):
        for half in (0, 1):
            own_kv(h, half)
    loads[2].wait()
    for n in range(4):
        q_ref[8 * n:8 * n + 8] = jnp.swapaxes(q_raw[:, 8 * n:8 * n + 8], 0, 1)

    def send_q(h, half):
        for d in (2, 3, 1):
            q_send(h, half, d).start()

    @pl.when(first)
    def _():
        send_q(1, 1)

    send_q(0, 0)
    send_q(0, 1)
    send_q(1, 0)

    @pl.when(jnp.logical_not(first))
    def _():
        send_q(1, 1)

    for h in (0, 1):
        for half in (0, 1):
            own_q(h, half)

    def relay_own(h):
        for half in (0, 1):
            if h == 1:
                z_each(h, half, 0, z_own)
            for d in (1, 2, 3):
                kv_both(h, half, d).wait_recv()
                z_each(h, half, d, z_own)

    order = words(z, PUMP, 4)

    def z_fwd(h, b, way):
        ref = kvb.at[h, b]
        return remote(ref, ref, f_s.at[h, b], z_r.at[h, b], z_dev(way))

    def fwd_ways(h, b):
        from_up = jnp.logical_and(b > z, b < 7 - z)
        down = jnp.logical_and(from_up, jnp.logical_or(z > 1, jnp.logical_and(second, h == 0)))
        up = jnp.logical_or(jnp.logical_and(has_up, b < z), jnp.logical_and(second, b == 7))
        return up, down

    def pump(i, _):
        code = entry(order, i, 4)
        h, b = code // 8, code % 8
        ref = kvb.at[h, b]
        remote(ref, ref, f_s.at[h, b], z_r.at[h, b], (dp, z, partners[1])).wait_recv()
        up, down = fwd_ways(h, b)

        @pl.when(down)
        def _():
            z_fwd(h, b, 1).start()

        @pl.when(up)
        def _():
            z_fwd(h, b, 0).start()

        return 0

    def fwd_wait(i, _):
        code = entry(order, i, 4)
        h, b = code // 8, code % 8
        up, down = fwd_ways(h, b)

        @pl.when(jnp.logical_or(up, down))
        def _():
            ref = kvb.at[h, b]
            remote(ref, ref, f_s.at[h, b], z_r.at[h, b], (dp, z, partners[1])).wait_send()

        return 0

    def chain(items, kk, vv):
        def scores(it):
            tile, nk, _, _ = it
            return lax.dot_general(qb[tile], kk[:nk], (((1,), (1,)), ((), ())), preferred_element_type=jnp.float32)

        def value(pend):
            tile, nk, p, alpha = pend
            pv = jnp.dot(p, vv[:nk], preferred_element_type=jnp.float32)
            ab[tile] = pv if alpha is None else alpha * ab[tile] + pv

        s = scores(items[0])
        pend = None
        for n, it in enumerate(items):
            nxt = scores(items[n + 1]) if n + 1 < len(items) else None
            tile, nk, mask, begins = it
            if mask is not None:
                s = jnp.where(mask, s, NEG)
            m = jnp.max(s, axis=1, keepdims=True)
            if begins:
                m = jnp.broadcast_to(m, (256, HD))
                alpha = None
            else:
                old = mb[tile]
                m = jnp.maximum(old, m)
                alpha = jnp.exp2((old - m) * c)
            mb[tile] = m
            p = jnp.exp2((s - jnp.concatenate([m] * (nk // HD), axis=1)) * c)
            tot = p[:, :HD]
            for j in range(1, nk // HD):
                tot = tot + p[:, j * HD:(j + 1) * HD]
            lb[tile] = tot if begins else alpha * lb[tile] + tot
            if pend is not None:
                value(pend)
            pend = (tile, nk, p.astype(jnp.bfloat16), alpha)
            s = nxt
        value(pend)

    def full(g, n, h, b):
        chain([(g * 4 + t, B, None, False) for t in range(n)], kvb.at[h, b, 0], kvb.at[h, b, 1])

    def diag(g, h, b, lower, begins):
        items = []
        for t, low in enumerate(lower):
            nk = 512 if low else 256
            row = lax.broadcasted_iota(jnp.int32, (256, nk), 0) + (256 if low else 0)
            mask = lax.broadcasted_iota(jnp.int32, (256, nk), 1) <= row
            items.append((g * 4 + t, nk, mask, begins))
        chain(items, kvb.at[h, b, 0], kvb.at[h, b, 1])

    def o_own(h, half):
        return pltpu.make_async_copy(
            rows4(ob, h, half, cx),
            o_ref.at[pl.ds(8 * cx + 4 * h, 4), pl.ds(half * S, S)], oloc.at[h, half])

    for t in range(32, 36):
        mb[t] = jnp.full((256, HD), NEG, jnp.float32)
        lb[t] = jnp.zeros((256, HD), jnp.float32)
        ab[t] = jnp.zeros((256, HD), jnp.float32)
    relay_own(0)
    count = [len(p) for p in PROGRAM]
    ops = words(z, [[op | g << 3 | b << 7 | n << 10 for op, g, b, n in p] for p in PROGRAM], 14)

    def run(i, at):
        code = entry(ops, i, 14)
        op, gc, b, upto = code % 8, (code // 8) % 16, (code // 128) % 8, code // 1024
        h = jnp.where(gc < 4, 0, 1)
        half = (gc // 2) % 2
        other = gc % 2
        extra = gc == X
        y = jnp.where(other == 0, cx // 2, 1 - cx // 2)
        g = jnp.where(extra, 8, gc - other + y)
        lax.fori_loop(at, upto, pump, 0)

        @pl.when(op == FULL)
        def _():
            full(g, 4, h, b)

        @pl.when(op == PAIR)
        def _():
            full(gc, 8, h, b)

        @pl.when(op == TRIO)
        def _():
            full(H1, 12, 1, b)

        @pl.when(op == DIAG)
        def _():
            lower = jnp.where(half == 0, y == 1, y == 0)

            @pl.when(extra)
            def _():
                diag(8, 1, 7, (True, True, False, False), False)

            @pl.when(jnp.logical_not(extra))
            def _():
                @pl.when(other == 0)
                def _():
                    q_both(h, half, 1).wait_recv()

                @pl.when(other == 1)
                def _():
                    q_both(h, half, 2).wait_recv()
                    q_both(h, half, 3).wait_recv()

                @pl.when(lower)
                def _():
                    diag(g, h, b, (True,) * 4, True)

                @pl.when(jnp.logical_not(lower))
                def _():
                    diag(g, h, b, (False,) * 4, True)

        @pl.when(op == FIN)
        def _():
            for t in range(4):
                tile = g * 4 + t
                ob[tile] = (ab[tile] / jnp.sum(lb[tile], axis=1, keepdims=True)).astype(jnp.bfloat16)

            @pl.when(extra)
            def _():
                for d in (2, 3, 1, 0):
                    xo_send(d).start()

            @pl.when(jnp.logical_not(extra))
            def _():
                @pl.when(other == 0)
                def _():
                    o_send(h, half, 1).start()
                    o_own(h, half).start()

                @pl.when(other == 1)
                def _():
                    o_send(h, half, 2).start()
                    o_send(h, half, 3).start()

        @pl.when(op == OTHER)
        def _():
            @pl.when(b == 0)
            def _():
                relay_own(1)

            @pl.when(b == 1)
            def _():
                for d in (1, 2, 3):
                    q_both(1, 1, d).wait_recv()
                for n in (1, 0):
                    x_send(n)

            @pl.when(b == 2)
            def _():
                for d in range(4):
                    z_own(1, 1, d, 0)

            @pl.when(b == 3)
            def _():
                x_both(0).wait_recv()

        return upto

    lax.fori_loop(0, pick(z, count), run, jnp.int32(0))

    lax.fori_loop(0, pick(z, [len(p) for p in PUMP]), fwd_wait, 0)

    def z_wait(h, half, d, way):
        z_piece(h, half, d, way).wait_send()

    for h in (0, 1):
        for half in (0, 1):
            for d in (1, 2, 3):
                kv_both(h, half, d).wait_send()
                q_send(h, half, d).wait_send()
            for d in range(4):
                z_each(h, half, d, z_wait)
                if (h, half) == (1, 1):
                    @pl.when(z < 2)
                    def _():
                        z_wait(h, half, d, 0)

            def o_wait():
                o_own(h, half).wait()
                for d in (1, 2, 3):
                    o_send(h, half, d).wait_send()
                    o_recv(h, half, d).wait_recv()

            if (h, half) == (1, 1):
                pl.when(jnp.logical_not(first))(o_wait)
            else:
                o_wait()

    @pl.when(first)
    def _():
        for n in (0, 1):
            x_both(n).wait_send()
            for d in range(4):
                xo_recv(n, d).wait_recv()

    @pl.when(has_x)
    def _():
        for d in range(4):
            xo_send(d).wait_send()


def by_rows(x_ref, o_ref):
    for n in range(4):
        o_ref[:, 8 * n:8 * n + 8] = jnp.swapaxes(x_ref[8 * n:8 * n + 8], 0, 1)


def solution(mesh):
    spec = P(("dp", "cy", "cx"))

    def local(q, k, v):
        dma = pltpu.SemaphoreType.DMA
        out = pl.pallas_call(
            kernel,
            out_shape=jax.ShapeDtypeStruct((32, 256, HD), jnp.bfloat16),
            in_specs=[pl.BlockSpec(memory_space=pl.ANY)] * 3,
            out_specs=pl.BlockSpec(memory_space=pl.ANY),
            scratch_shapes=[
                pltpu.VMEM((256, 32, HD), jnp.bfloat16),
                pltpu.VMEM((256, 8, HD), jnp.bfloat16),
                pltpu.VMEM((256, 8, HD), jnp.bfloat16),
                pltpu.VMEM((32, 256, HD), jnp.bfloat16),
                pltpu.VMEM((8, 256, HD), jnp.bfloat16),
                pltpu.VMEM((8, 256, HD), jnp.bfloat16),
                pltpu.VMEM((36, 256, HD), jnp.bfloat16),
                pltpu.VMEM((2, 8, 2, B, HD), jnp.bfloat16),
                pltpu.VMEM((36, 256, HD), jnp.bfloat16),
                pltpu.VMEM((36, 256, HD), jnp.float32),
                pltpu.VMEM((36, 256, HD), jnp.float32),
                pltpu.VMEM((36, 256, HD), jnp.float32),
                dma((2, 2, 3)), dma((2, 2, 3)),
                dma((2, 2, 3)), dma((2, 2, 3)),
                dma((2, 2, 4, 2)), dma((2, 8)), dma((2, 8)),
                dma((2, 2, 3)), dma((2, 2, 3)),
                dma((2,)), dma((1,)), dma((4,)), dma((2, 4)),
                dma((3,)), dma((2, 2)),
            ],
            compiler_params=pltpu.CompilerParams(
                collective_id=0, has_side_effects=True, vmem_limit_bytes=60 * 1024 * 1024),
        )(q, k, v)
        return pl.pallas_call(
            by_rows,
            grid=(2,),
            out_shape=jax.ShapeDtypeStruct((256, 32, HD), jnp.bfloat16),
            in_specs=[pl.BlockSpec((32, S, HD), lambda i: (0, i, 0))],
            out_specs=pl.BlockSpec((S, 32, HD), lambda i: (i, 0, 0)),
        )(out)

    return jax.shard_map(local, mesh=mesh, in_specs=(spec, spec, spec), out_specs=spec, check_vma=False)
```

```python
import jax
import jax.numpy as jnp
from jax import lax
from jax.experimental import pallas as pl
from jax.experimental.pallas import tpu as pltpu
from jax.sharding import PartitionSpec as P

MESH = pl.DeviceIdType.MESH
NEG = -1.0e30
LOG2E = 1.4426950408889634
B = 512
S = 128
HD = 128

PUMP = (
    (1, 6, 2, 5, 3, 4,),
    (0, 2, 5, 3, 8, 4, 10, 15, 13, 11, 12,),
    (1, 3, 4, 0, 11, 9, 12, 8, 15, 14,),
    (2, 1, 10, 0, 9, 8,),
)
FULL, DIAG, FIN, OTHER, FULL2, FULL3 = range(6)
X = 8
PROGRAM = (
    ((1, 0, 0, 0), (2, 0, 0, 0), (1, 0, 2, 7), (4, 1, 2, 1, 2, 0), (3, 2, 0, 0), (0, 2, 2, 6), (1, 2, 4, 0),
     (2, 2, 4, 0), (3, 3, 0, 1), (3, 3, 0, 2), (0, 3, 2, 2), (1, 4, 1, 0), (2, 4, 1, 0), (0, 4, 2, 5),
     (1, 5, 3, 7), (4, 5, 3, 1, 3, 2), (4, 5, 3, 3, 3, 5), (4, 5, 3, 6, 3, 0), (4, 6, 3, 4, 2, 3),
     (2, 6, 3, 0), (1, 6, 5, 0), (2, 6, 5, 0), (0, 6, 2, 4), (2, 6, 2, 0),),
    ((1, 0, 0, 1), (0, 1, 0, 0), (2, 2, 0, 0), (1, 2, 2, 6), (4, 2, 2, 0, 2, 2), (0, 2, 2, 1), (3, 3, 0, 0),
     (0, 3, 2, 5), (1, 3, 4, 1), (1, 3, 6, 6), (0, 3, 6, 1), (1, 4, 1, 1), (4, 4, 1, 0, 2, 3), (2, 5, 1, 0),
     (4, 5, 4, 0, 6, 0), (2, 5, 4, 0), (1, 6, 3, 6), (4, 6, 3, 0, 3, 2), (4, 6, 3, 3, 3, 4),
     (4, 6, 3, 5, 3, 1), (2, 7, 3, 0), (1, 7, 5, 1), (4, 7, 5, 0, 2, 4), (3, 8, 0, 2), (2, 8, 5, 0),
     (2, 8, 2, 0), (0, 8, 6, 2), (1, 9, 7, 6), (4, 9, 7, 0, 7, 2), (3, 9, 0, 3), (4, 9, 8, 0, 8, 2),
     (4, 9, 8, 5, 8, 1), (4, 10, 8, 3, 8, 6), (1, 10, 8, 7), (4, 10, 7, 3, 7, 5), (4, 11, 8, 4, 7, 4),
     (2, 11, 8, 0), (4, 11, 7, 1, 6, 3), (2, 11, 7, 0), (4, 11, 6, 4, 6, 5), (2, 11, 6, 0),),
    ((1, 0, 0, 2), (0, 1, 0, 1), (1, 2, 2, 5), (4, 2, 2, 1, 2, 3), (0, 2, 2, 2), (3, 3, 0, 0), (0, 3, 2, 4),
     (1, 3, 4, 2), (1, 3, 6, 5), (4, 4, 0, 0, 2, 0), (2, 4, 0, 0), (1, 4, 1, 2), (4, 4, 1, 0, 1, 1),
     (2, 5, 1, 0), (2, 6, 2, 0), (4, 6, 4, 1, 6, 1), (1, 6, 3, 5), (4, 6, 3, 0, 3, 1), (4, 7, 3, 3, 3, 4),
     (4, 7, 3, 2, 6, 3), (2, 7, 3, 0), (1, 7, 5, 2), (4, 7, 5, 1, 6, 4), (4, 8, 5, 0, 4, 0), (2, 8, 5, 0),
     (1, 8, 7, 5), (4, 8, 7, 0, 7, 1), (4, 8, 7, 3, 7, 4), (4, 8, 7, 2, 6, 0), (3, 9, 0, 3),
     (4, 9, 8, 0, 8, 1), (4, 9, 8, 3, 8, 4), (1, 9, 8, 7), (4, 9, 8, 2, 8, 5), (4, 10, 8, 6, 6, 2),
     (2, 10, 8, 0), (2, 10, 7, 0), (2, 10, 4, 0), (2, 10, 6, 0),),
    ((1, 0, 0, 3), (0, 1, 0, 2), (1, 1, 2, 4), (4, 1, 2, 2, 2, 3), (3, 1, 0, 0), (1, 1, 4, 3), (1, 1, 6, 4),
     (0, 1, 6, 3), (4, 2, 0, 1, 2, 1), (1, 2, 1, 3), (4, 2, 1, 1, 1, 2), (4, 3, 4, 2, 6, 2), (1, 3, 3, 4),
     (4, 3, 3, 1, 3, 2), (4, 4, 1, 0, 3, 0), (2, 4, 1, 0), (4, 4, 3, 3, 0, 0), (2, 4, 3, 0), (1, 4, 5, 3),
     (4, 4, 5, 2, 2, 0), (4, 5, 5, 1, 4, 1), (1, 5, 7, 4), (4, 5, 7, 1, 7, 2), (4, 5, 7, 3, 6, 1),
     (2, 5, 0, 0), (2, 5, 2, 0), (4, 6, 5, 0, 7, 0), (2, 6, 5, 0), (2, 6, 7, 0), (4, 6, 4, 0, 6, 0),
     (2, 6, 4, 0), (2, 6, 6, 0),),
)


def encode(op, taken, *pairs):
    word = op | taken << 3
    for n in range(0, len(pairs), 2):
        word |= (pairs[n] | pairs[n + 1] << 4) << (7 + 7 * (n // 2))
    return word


def pick(z, values):
    out = jnp.int32(values[0])
    for i in range(1, len(values)):
        out = jnp.where(z == i, jnp.int32(values[i]), out)
    return out


def words(z, seqs, bits):
    per = 31 // bits
    n = max(len(q) for q in seqs)
    return [pick(z, [sum(x << (bits * i) for i, x in enumerate(q[w:w + per])) for q in seqs])
            for w in range(0, n, per)]


def entry(table, i, bits):
    per = 31 // bits
    word = table[0]
    for w in range(1, len(table)):
        word = jnp.where(i >= per * w, table[w], word)
    return lax.shift_right_logical(word, bits * (i % per)) & ((1 << bits) - 1)


def kernel(q_in, k_in, v_in, o_ref, q_raw, k_raw, v_raw, q_ref, k_ref, v_ref, qb, kvb, ob, mb, lb, ab,
           kv_s, kv_r, q_s, q_r, z_s, z_r, f_s, o_s, o_r, x_s, x_r, xo_s, xo_r, loc, oloc):
    dp = lax.axis_index("dp")
    z = lax.axis_index("cy")
    cx = lax.axis_index("cx")
    c = (HD ** -0.5) * LOG2E
    partners = (cx, cx + 1 - 2 * (cx % 2), (cx + 2) % 4, 3 - cx)
    first, second = z == 0, z == 1
    has_dn, has_up = z > 0, z < 3
    has_x = jnp.logical_and(z >= 1, z <= 2)

    def span_at(half, who):
        return (who if half == 0 else 3 - who) * S

    def blk(half):
        return z if half == 0 else 7 - z

    def remote(src, dst, ssem, rsem, dev):
        return pltpu.make_async_remote_copy(src, dst, ssem, rsem, device_id=dev, device_id_type=MESH)

    def kv_piece(h, half, who):
        return kvb.at[h, blk(half), :, pl.ds(span_at(half, who), S)]

    def kv_send(h, half, d):
        t = partners[d]
        for ref, n in ((k_ref, 0), (v_ref, 1)):
            remote(ref.at[2 * t + h, pl.ds(half * S, S)], kvb.at[h, blk(half), n, pl.ds(span_at(half, cx), S)],
                   kv_s.at[h, half, d - 1], kv_r.at[h, half, d - 1], (dp, z, t)).start()

    def kv_both(h, half, d):
        ref = kv_piece(h, half, partners[d])
        return remote(ref, ref, kv_s.at[h, half, d - 1], kv_r.at[h, half, d - 1], (dp, z, partners[d]))

    def rows4(ref, h, half, who):
        at = jnp.where(half == 0, who % 2, 1 - who % 2) * S
        return ref.at[pl.ds(((h * 2 + half) * 2 + who // 2) * 4, 4), pl.ds(at, S)]

    def q_piece(h, half, who):
        return rows4(qb, h, half, who)

    def q_send(h, half, d):
        t = partners[d]
        return remote(q_ref.at[pl.ds(8 * t + 4 * h, 4), pl.ds(half * S, S)], q_piece(h, half, cx),
                      q_s.at[h, half, d - 1], q_r.at[h, half, d - 1], (dp, z, t))

    def q_both(h, half, d):
        ref = q_piece(h, half, partners[d])
        return remote(ref, ref, q_s.at[h, half, d - 1], q_r.at[h, half, d - 1], (dp, z, partners[d]))

    def o_send(h, half, d):
        t = partners[d]
        return remote(rows4(ob, h, half, t),
                      o_ref.at[pl.ds(8 * cx + 4 * h, 4), pl.ds(half * S, S)],
                      o_s.at[h, half, d - 1], o_r.at[h, half, d - 1], (dp, z, t))

    def o_recv(h, half, d):
        t = partners[d]
        ref = o_ref.at[pl.ds(8 * t + 4 * h, 4), pl.ds(half * S, S)]
        return remote(ref, ref, o_s.at[h, half, d - 1], o_r.at[h, half, d - 1], (dp, z, t))

    def x_send(n):
        for y in (0, 1):
            remote(qb.at[pl.ds((6 + y) * 4 + 2 * n, 2)], qb.at[pl.ds(32 + 2 * y, 2)],
                   x_s.at[n], x_r.at[0], (dp, n + 1, cx)).start()

    def x_both(n):
        ref = qb.at[pl.ds(32, 4)]
        return remote(ref, ref, x_s.at[n], x_r.at[0], (dp, 0, cx))

    def xo_send(d):
        t = partners[d]
        return remote(ob.at[pl.ds(32 + 2 * (t // 2), 2), pl.ds((1 - t % 2) * S, S)],
                      o_ref.at[pl.ds(8 * cx + 2 + 2 * z, 2), pl.ds(S, S)],
                      xo_s.at[d], xo_r.at[z - 1, d], (dp, 0, t))

    def xo_recv(n, d):
        ref = o_ref.at[pl.ds(8 * partners[d] + 4 + 2 * n, 2), pl.ds(S, S)]
        return remote(ref, ref, xo_s.at[d], xo_r.at[n, d], (dp, n + 1, partners[d]))

    def z_dev(way):
        return (dp, z + 1 if way == 0 else z - 1, cx)

    def z_own(h, half, d, way):
        b = blk(half)
        if d == 0:
            for ref, n in ((k_ref, 0), (v_ref, 1)):
                remote(ref.at[2 * cx + h, pl.ds(half * S, S)], kvb.at[h, b, n, pl.ds(span_at(half, cx), S)],
                       z_s.at[h, half, d, way], z_r.at[h, b], z_dev(way)).start()
        else:
            z_piece(h, half, d, way).start()

    def z_piece(h, half, d, way):
        ref = kv_piece(h, half, partners[d])
        return remote(ref, ref, z_s.at[h, half, d, way], z_r.at[h, blk(half)], z_dev(way))

    def z_cond(h, half, way):
        if way == 0:
            return has_up if half == 0 else None
        return has_dn if h == 0 else z > 1

    def z_each(h, half, d, do):
        for way in (0, 1):
            cond = z_cond(h, half, way)
            if cond is not None:
                @pl.when(cond)
                def _():
                    do(h, half, d, way)

    def own_kv(h, half):
        for ref, n in ((k_ref, 0), (v_ref, 1)):
            kvb[h, blk(half), n, pl.ds(span_at(half, cx), S)] = ref[2 * cx + h, half * S:(half + 1) * S]

    def own_q(h, half):
        at = (cx % 2 if half == 0 else 1 - cx % 2) * S
        for t in range(4):
            qb[((h * 2 + half) * 2 + cx // 2) * 4 + t, pl.ds(at, S)] = q_ref[8 * cx + 4 * h + t, half * S:(half + 1) * S]

    loads = [pltpu.make_async_copy(src, dst, loc.at[n])
             for n, (src, dst) in enumerate(((k_in, k_raw), (v_in, v_raw), (q_in, q_raw)))]
    for copy in loads:
        copy.start()

    barrier = pltpu.get_barrier_semaphore()
    for n in range(1, 16):
        other = (z * 4 + cx + n) % 16
        pl.semaphore_signal(barrier, inc=1, device_id=(dp, other // 4, other % 4), device_id_type=MESH)
    for copy, src, dst in zip(loads[:2], (k_raw, v_raw), (k_ref, v_ref)):
        copy.wait()
        dst[...] = jnp.swapaxes(src[...], 0, 1)
    pl.semaphore_wait(barrier, 15)

    for h in (0, 1):
        for half in (0, 1):
            for d in (2, 3, 1):
                kv_send(h, half, d)
            if h == 0:
                z_each(h, half, 0, z_own)

    for h in (0, 1):
        for half in (0, 1):
            own_kv(h, half)
    loads[2].wait()
    for n in range(4):
        q_ref[8 * n:8 * n + 8] = jnp.swapaxes(q_raw[:, 8 * n:8 * n + 8], 0, 1)

    def send_q(h, half):
        for d in (2, 3, 1):
            q_send(h, half, d).start()

    @pl.when(first)
    def _():
        send_q(1, 1)

    send_q(0, 0)
    send_q(0, 1)
    send_q(1, 0)

    @pl.when(jnp.logical_not(first))
    def _():
        send_q(1, 1)

    for h in (0, 1):
        for half in (0, 1):
            own_q(h, half)

    def relay_own(h):
        for half in (0, 1):
            if h == 1:
                z_each(h, half, 0, z_own)
            for d in (1, 2, 3):
                kv_both(h, half, d).wait_recv()
                z_each(h, half, d, z_own)

    order = words(z, PUMP, 4)

    def z_fwd(h, b, way):
        ref = kvb.at[h, b]
        return remote(ref, ref, f_s.at[h, b], z_r.at[h, b], z_dev(way))

    def fwd_ways(h, b):
        from_up = jnp.logical_and(b > z, b < 7 - z)
        down = jnp.logical_and(from_up, jnp.logical_or(z > 1, jnp.logical_and(second, h == 0)))
        up = jnp.logical_or(jnp.logical_and(has_up, b < z), jnp.logical_and(second, b == 7))
        return up, down

    def pump(i, _):
        code = entry(order, i, 4)
        h, b = code // 8, code % 8
        ref = kvb.at[h, b]
        remote(ref, ref, f_s.at[h, b], z_r.at[h, b], (dp, z, partners[1])).wait_recv()
        up, down = fwd_ways(h, b)

        @pl.when(down)
        def _():
            z_fwd(h, b, 1).start()

        @pl.when(up)
        def _():
            z_fwd(h, b, 0).start()

        return 0

    def fwd_wait(i, _):
        code = entry(order, i, 4)
        h, b = code // 8, code % 8
        up, down = fwd_ways(h, b)

        @pl.when(jnp.logical_or(up, down))
        def _():
            ref = kvb.at[h, b]
            remote(ref, ref, f_s.at[h, b], z_r.at[h, b], (dp, z, partners[1])).wait_send()

        return 0

    def chain(items):
        def scores(it):
            tile, h, b, nk, _, _ = it
            return lax.dot_general(qb[tile], kvb[h, b, 0, :nk], (((1,), (1,)), ((), ())), preferred_element_type=jnp.float32)

        def value(pend):
            tile, h, b, nk, p, alpha = pend
            pv = jnp.dot(p, kvb[h, b, 1, :nk], preferred_element_type=jnp.float32)
            ab[tile] = pv if alpha is None else alpha * ab[tile] + pv

        s = scores(items[0])
        pend = None
        for n, it in enumerate(items):
            nxt = scores(items[n + 1]) if n + 1 < len(items) else None
            tile, h, b, nk, mask, begins = it
            if mask is not None:
                s = jnp.where(mask, s, NEG)
            m = jnp.max(s, axis=1, keepdims=True)
            if begins:
                m = jnp.broadcast_to(m, (256, HD))
                alpha = None
            else:
                old = mb[tile]
                m = jnp.maximum(old, m)
                alpha = jnp.exp2((old - m) * c)
            mb[tile] = m
            p = jnp.exp2((s - jnp.concatenate([m] * (nk // HD), axis=1)) * c)
            tot = p[:, :HD]
            for j in range(1, nk // HD):
                tot = tot + p[:, j * HD:(j + 1) * HD]
            lb[tile] = tot if begins else alpha * lb[tile] + tot
            if pend is not None:
                value(pend)
            pend = (tile, h, b, nk, p.astype(jnp.bfloat16), alpha)
            s = nxt
        value(pend)

    def full(parts):
        chain([(g * 4 + t, h, b, B, None, False) for g, h, b in parts for t in range(4)])

    def diag(g, h, b, lower, begins):
        items = []
        for t, low in enumerate(lower):
            nk = 512 if low else 256
            row = lax.broadcasted_iota(jnp.int32, (256, nk), 0) + (256 if low else 0)
            mask = lax.broadcasted_iota(jnp.int32, (256, nk), 1) <= row
            items.append((g * 4 + t, h, b, nk, mask, begins))
        chain(items)

    def o_own(h, half):
        return pltpu.make_async_copy(
            rows4(ob, h, half, cx),
            o_ref.at[pl.ds(8 * cx + 4 * h, 4), pl.ds(half * S, S)], oloc.at[h, half])

    for t in range(32, 36):
        mb[t] = jnp.full((256, HD), NEG, jnp.float32)
        lb[t] = jnp.zeros((256, HD), jnp.float32)
        ab[t] = jnp.zeros((256, HD), jnp.float32)
    relay_own(0)
    count = [len(p) for p in PROGRAM]
    ops = words(z, [[encode(*item) for item in p] for p in PROGRAM], 28)

    def run(i, at):
        code = entry(ops, i, 28)
        op, upto = code % 8, (code // 8) % 16
        parts = []
        for n in range(3):
            gc, b = (code // 128 ** (n + 1)) % 16, (code // (16 * 128 ** (n + 1))) % 8
            y = jnp.where(gc % 2 == 0, cx // 2, 1 - cx // 2)
            parts.append((jnp.where(gc == X, X, gc - gc % 2 + y), jnp.where(gc < 4, 0, 1), b))
        gc, b = (code // 128) % 16, (code // 2048) % 8
        half, other, extra = (gc // 2) % 2, gc % 2, gc == X
        y = jnp.where(other == 0, cx // 2, 1 - cx // 2)
        g, h, _ = parts[0]
        lax.fori_loop(at, upto, pump, 0)

        for n, name in ((1, FULL), (2, FULL2), (3, FULL3)):
            @pl.when(op == name)
            def _():
                full(parts[:n])

        @pl.when(op == DIAG)
        def _():
            lower = jnp.where(half == 0, y == 1, y == 0)

            @pl.when(extra)
            def _():
                diag(8, 1, 7, (True, True, False, False), False)

            @pl.when(jnp.logical_not(extra))
            def _():
                @pl.when(other == 0)
                def _():
                    q_both(h, half, 1).wait_recv()

                @pl.when(other == 1)
                def _():
                    q_both(h, half, 2).wait_recv()
                    q_both(h, half, 3).wait_recv()

                @pl.when(lower)
                def _():
                    diag(g, h, b, (True,) * 4, True)

                @pl.when(jnp.logical_not(lower))
                def _():
                    diag(g, h, b, (False,) * 4, True)

        @pl.when(op == FIN)
        def _():
            for t in range(4):
                tile = g * 4 + t
                ob[tile] = (ab[tile] / jnp.sum(lb[tile], axis=1, keepdims=True)).astype(jnp.bfloat16)

            @pl.when(extra)
            def _():
                for d in (2, 3, 1, 0):
                    xo_send(d).start()

            @pl.when(jnp.logical_not(extra))
            def _():
                @pl.when(other == 0)
                def _():
                    o_send(h, half, 1).start()
                    o_own(h, half).start()

                @pl.when(other == 1)
                def _():
                    o_send(h, half, 2).start()
                    o_send(h, half, 3).start()

        @pl.when(op == OTHER)
        def _():
            @pl.when(b == 0)
            def _():
                relay_own(1)

            @pl.when(b == 1)
            def _():
                for d in (1, 2, 3):
                    q_both(1, 1, d).wait_recv()
                for n in (1,):
                    x_send(n)

            @pl.when(b == 2)
            def _():
                for d in range(4):
                    z_own(1, 1, d, 0)

                @pl.when(first)
                def _():
                    x_send(0)

            @pl.when(b == 3)
            def _():
                x_both(0).wait_recv()

        return upto

    lax.fori_loop(0, pick(z, count), run, jnp.int32(0))

    lax.fori_loop(0, pick(z, [len(p) for p in PUMP]), fwd_wait, 0)

    def z_wait(h, half, d, way):
        z_piece(h, half, d, way).wait_send()

    for h in (0, 1):
        for half in (0, 1):
            for d in (1, 2, 3):
                kv_both(h, half, d).wait_send()
                q_send(h, half, d).wait_send()
            for d in range(4):
                z_each(h, half, d, z_wait)
                if (h, half) == (1, 1):
                    @pl.when(z < 2)
                    def _():
                        z_wait(h, half, d, 0)

            def o_wait():
                o_own(h, half).wait()
                for d in (1, 2, 3):
                    o_send(h, half, d).wait_send()
                    o_recv(h, half, d).wait_recv()

            if (h, half) == (1, 1):
                pl.when(jnp.logical_not(first))(o_wait)
            else:
                o_wait()

    @pl.when(first)
    def _():
        for n in (0, 1):
            x_both(n).wait_send()
            for d in range(4):
                xo_recv(n, d).wait_recv()

    @pl.when(has_x)
    def _():
        for d in range(4):
            xo_send(d).wait_send()


PARTS = 8


def by_rows(x_ref, o_ref, x_in, out, in_sem, out_sem):
    rows = 256 // PARTS

    def fetch(n):
        at = pl.ds(n * rows, rows)
        return pltpu.make_async_copy(x_ref.at[:, at], x_in.at[n], in_sem.at[n])

    def put(n):
        at = pl.ds(n * rows, rows)
        return pltpu.make_async_copy(out.at[at], o_ref.at[at], out_sem.at[n])

    for n in range(PARTS):
        fetch(n).start()
    for n in range(PARTS):
        fetch(n).wait()
        for g in range(4):
            out[n * rows:(n + 1) * rows, 8 * g:8 * g + 8] = jnp.swapaxes(x_in[n, 8 * g:8 * g + 8], 0, 1)
        put(n).start()
    for n in range(PARTS):
        put(n).wait()


def solution(mesh):
    spec = P(("dp", "cy", "cx"))

    def local(q, k, v):
        dma = pltpu.SemaphoreType.DMA
        out = pl.pallas_call(
            kernel,
            out_shape=jax.ShapeDtypeStruct((32, 256, HD), jnp.bfloat16),
            in_specs=[pl.BlockSpec(memory_space=pl.ANY)] * 3,
            out_specs=pl.BlockSpec(memory_space=pl.ANY),
            scratch_shapes=[
                pltpu.VMEM((256, 32, HD), jnp.bfloat16),
                pltpu.VMEM((256, 8, HD), jnp.bfloat16),
                pltpu.VMEM((256, 8, HD), jnp.bfloat16),
                pltpu.VMEM((32, 256, HD), jnp.bfloat16),
                pltpu.VMEM((8, 256, HD), jnp.bfloat16),
                pltpu.VMEM((8, 256, HD), jnp.bfloat16),
                pltpu.VMEM((36, 256, HD), jnp.bfloat16),
                pltpu.VMEM((2, 8, 2, B, HD), jnp.bfloat16),
                pltpu.VMEM((36, 256, HD), jnp.bfloat16),
                pltpu.VMEM((36, 256, HD), jnp.float32),
                pltpu.VMEM((36, 256, HD), jnp.float32),
                pltpu.VMEM((36, 256, HD), jnp.float32),
                dma((2, 2, 3)), dma((2, 2, 3)),
                dma((2, 2, 3)), dma((2, 2, 3)),
                dma((2, 2, 4, 2)), dma((2, 8)), dma((2, 8)),
                dma((2, 2, 3)), dma((2, 2, 3)),
                dma((2,)), dma((1,)), dma((4,)), dma((2, 4)),
                dma((3,)), dma((2, 2)),
            ],
            compiler_params=pltpu.CompilerParams(
                collective_id=0, has_side_effects=True, vmem_limit_bytes=60 * 1024 * 1024),
        )(q, k, v)
        return pl.pallas_call(
            by_rows,
            out_shape=jax.ShapeDtypeStruct((256, 32, HD), jnp.bfloat16),
            in_specs=[pl.BlockSpec(memory_space=pl.ANY)],
            out_specs=pl.BlockSpec(memory_space=pl.ANY),
            scratch_shapes=[
                pltpu.VMEM((PARTS, 32, 256 // PARTS, HD), jnp.bfloat16),
                pltpu.VMEM((256, 32, HD), jnp.bfloat16),
                dma((PARTS,)), dma((PARTS,)),
            ],
            compiler_params=pltpu.CompilerParams(vmem_limit_bytes=60 * 1024 * 1024),
        )(out)

    return jax.shard_map(local, mesh=mesh, in_specs=(spec, spec, spec), out_specs=spec, check_vma=False)
```

```python
import jax
import jax.numpy as jnp
from jax import lax
from jax.experimental import pallas as pl
from jax.experimental.pallas import tpu as pltpu
from jax.sharding import PartitionSpec as P

MESH = pl.DeviceIdType.MESH
NEG = -1.0e30
LOG2E = 1.4426950408889634
B = 512
S = 128
HD = 128

PUMP = (
    (1, 6, 2, 5, 3, 4,),
    (0, 2, 5, 3, 8, 4, 10, 15, 13, 11, 12,),
    (1, 3, 4, 0, 11, 9, 12, 8, 15, 14,),
    (2, 1, 10, 0, 9, 8,),
)
FULL, DIAG, FIN, OTHER, FULL2, FULL3 = range(6)
X = 8
PROGRAM = (
    (0x3901, 0x100, 0x908, 0x9, 0xa, 0x13, 0x3110, 0x211, 0x212, 0x81b, 0x101b, 0x1118, 0x2920, 0xa1, 0xa2,
     0x1928, 0x39a9, 0x8c9ac, 0x14d9ac, 0xf1ac, 0x10e134, 0x132, 0x1b2, 0x2b1, 0x2b2,),
    (0x801, 0x8, 0x12, 0x3111, 0x88114, 0x910, 0x1b, 0xa19, 0x2918, 0x3319, 0xb18, 0x8a1, 0xc80a4, 0xaa,
     0x1822c, 0x22a, 0x31b1, 0x8c1b4, 0x10d9b4, 0x4e9b4, 0x1ba, 0x9a13c, 0x1043, 0x142, 0xac1, 0x2c0, 0x2ca,
     0x33c9, 0x9c3cc, 0x184b, 0xa044c, 0x62c4c, 0x1a1c54, 0x3c51, 0x15dbd4, 0x11e45c, 0x45a, 0xd8bdc, 0x3da,
     0x15a35c, 0x35a,),
    (0x1001, 0x808, 0x2911, 0xc8914, 0x1110, 0x1b, 0x2118, 0x2b19, 0x1318, 0x8024, 0x22, 0x122, 0x10a1,
     0x440a4, 0xd8b34, 0xb2, 0x29b1, 0x4c1b4, 0xce33c, 0x8e1bc, 0x12b9, 0xab8, 0x1ba, 0x182c4, 0x2c2, 0x342,
     0x2bc1, 0x5c3c4, 0x11dbc4, 0x184b, 0x6044c, 0x121c4c, 0x3c49, 0x16144c, 0x9f454, 0x452, 0x3d2, 0x1251,
     0x50254, 0x252,),
    (0x1801, 0x1008, 0x2109, 0xc910c, 0xb, 0x2309, 0x1b08, 0x1a09, 0x48814, 0x1891, 0x84894, 0x9131c, 0x2199,
     0x8c99c, 0x1998, 0xa4, 0xa2, 0x22, 0x81a4, 0x1a2, 0x50b2c, 0x12a, 0x23a9, 0x9cbac, 0x1ba8, 0x1aa9,
     0x94aac, 0x183b4, 0x3b2, 0x332, 0x14234, 0x232, 0x2b2,),
)


def pick(z, values):
    out = jnp.int32(values[0])
    for i in range(1, len(values)):
        out = jnp.where(z == i, jnp.int32(values[i]), out)
    return out


def words(z, seqs, bits):
    per = 31 // bits
    n = max(len(q) for q in seqs)
    return [pick(z, [sum(x << (bits * i) for i, x in enumerate(q[w:w + per])) for q in seqs])
            for w in range(0, n, per)]


def entry(table, i, bits):
    per = 31 // bits
    word = table[0]
    for w in range(1, len(table)):
        word = jnp.where(i >= per * w, table[w], word)
    return lax.shift_right_logical(word, bits * (i % per)) & ((1 << bits) - 1)


def kernel(q_in, k_in, v_in, o_ref, q_raw, k_raw, v_raw, q_ref, k_ref, v_ref, qb, kvb, ob, mb, lb, ab,
           kv_s, kv_r, q_s, q_r, z_s, z_r, f_s, o_s, o_r, x_s, x_r, xo_s, xo_r, loc, oloc):
    dp = lax.axis_index("dp")
    z = lax.axis_index("cy")
    cx = lax.axis_index("cx")
    c = (HD ** -0.5) * LOG2E
    partners = (cx, cx + 1 - 2 * (cx % 2), (cx + 2) % 4, 3 - cx)
    first, second = z == 0, z == 1
    has_dn, has_up = z > 0, z < 3
    has_x = jnp.logical_and(z >= 1, z <= 2)

    def span_at(half, who):
        return (who if half == 0 else 3 - who) * S

    def blk(half):
        return z if half == 0 else 7 - z

    def remote(src, dst, ssem, rsem, dev):
        return pltpu.make_async_remote_copy(src, dst, ssem, rsem, device_id=dev, device_id_type=MESH)

    def kv_piece(h, half, who):
        return kvb.at[h, blk(half), :, pl.ds(span_at(half, who), S)]

    def kv_send(h, half, d):
        t = partners[d]
        for ref, n in ((k_ref, 0), (v_ref, 1)):
            remote(ref.at[2 * t + h, pl.ds(half * S, S)], kvb.at[h, blk(half), n, pl.ds(span_at(half, cx), S)],
                   kv_s.at[h, half, d - 1], kv_r.at[h, half, d - 1], (dp, z, t)).start()

    def kv_both(h, half, d):
        ref = kv_piece(h, half, partners[d])
        return remote(ref, ref, kv_s.at[h, half, d - 1], kv_r.at[h, half, d - 1], (dp, z, partners[d]))

    def rows4(ref, h, half, who):
        at = jnp.where(half == 0, who % 2, 1 - who % 2) * S
        return ref.at[pl.ds(((h * 2 + half) * 2 + who // 2) * 4, 4), pl.ds(at, S)]

    def q_piece(h, half, who):
        return rows4(qb, h, half, who)

    def q_send(h, half, d):
        t = partners[d]
        return remote(q_ref.at[pl.ds(8 * t + 4 * h, 4), pl.ds(half * S, S)], q_piece(h, half, cx),
                      q_s.at[h, half, d - 1], q_r.at[h, half, d - 1], (dp, z, t))

    def q_both(h, half, d):
        ref = q_piece(h, half, partners[d])
        return remote(ref, ref, q_s.at[h, half, d - 1], q_r.at[h, half, d - 1], (dp, z, partners[d]))

    def o_send(h, half, d):
        t = partners[d]
        return remote(rows4(ob, h, half, t),
                      o_ref.at[pl.ds(8 * cx + 4 * h, 4), pl.ds(half * S, S)],
                      o_s.at[h, half, d - 1], o_r.at[h, half, d - 1], (dp, z, t))

    def o_recv(h, half, d):
        t = partners[d]
        ref = o_ref.at[pl.ds(8 * t + 4 * h, 4), pl.ds(half * S, S)]
        return remote(ref, ref, o_s.at[h, half, d - 1], o_r.at[h, half, d - 1], (dp, z, t))

    def x_send(n):
        for y in (0, 1):
            remote(qb.at[pl.ds((6 + y) * 4 + 2 * n, 2)], qb.at[pl.ds(32 + 2 * y, 2)],
                   x_s.at[n], x_r.at[0], (dp, n + 1, cx)).start()

    def x_both(n):
        ref = qb.at[pl.ds(32, 4)]
        return remote(ref, ref, x_s.at[n], x_r.at[0], (dp, 0, cx))

    def xo_send(d):
        t = partners[d]
        return remote(ob.at[pl.ds(32 + 2 * (t // 2), 2), pl.ds((1 - t % 2) * S, S)],
                      o_ref.at[pl.ds(8 * cx + 2 + 2 * z, 2), pl.ds(S, S)],
                      xo_s.at[d], xo_r.at[z - 1, d], (dp, 0, t))

    def xo_recv(n, d):
        ref = o_ref.at[pl.ds(8 * partners[d] + 4 + 2 * n, 2), pl.ds(S, S)]
        return remote(ref, ref, xo_s.at[d], xo_r.at[n, d], (dp, n + 1, partners[d]))

    def z_dev(way):
        return (dp, z + 1 if way == 0 else z - 1, cx)

    def z_own(h, half, d, way):
        b = blk(half)
        if d == 0:
            for ref, n in ((k_ref, 0), (v_ref, 1)):
                remote(ref.at[2 * cx + h, pl.ds(half * S, S)], kvb.at[h, b, n, pl.ds(span_at(half, cx), S)],
                       z_s.at[h, half, d, way], z_r.at[h, b], z_dev(way)).start()
        else:
            z_piece(h, half, d, way).start()

    def z_piece(h, half, d, way):
        ref = kv_piece(h, half, partners[d])
        return remote(ref, ref, z_s.at[h, half, d, way], z_r.at[h, blk(half)], z_dev(way))

    def z_cond(h, half, way):
        if way == 0:
            return has_up if half == 0 else None
        return has_dn if h == 0 else z > 1

    def z_each(h, half, d, do):
        for way in (0, 1):
            cond = z_cond(h, half, way)
            if cond is not None:
                @pl.when(cond)
                def _():
                    do(h, half, d, way)

    def own_kv(h, half):
        for ref, n in ((k_ref, 0), (v_ref, 1)):
            kvb[h, blk(half), n, pl.ds(span_at(half, cx), S)] = ref[2 * cx + h, half * S:(half + 1) * S]

    def own_q(h, half):
        at = (cx % 2 if half == 0 else 1 - cx % 2) * S
        for t in range(4):
            qb[((h * 2 + half) * 2 + cx // 2) * 4 + t, pl.ds(at, S)] = q_ref[8 * cx + 4 * h + t, half * S:(half + 1) * S]

    loads = [pltpu.make_async_copy(src, dst, loc.at[n])
             for n, (src, dst) in enumerate(((k_in, k_raw), (v_in, v_raw), (q_in, q_raw)))]
    for copy in loads:
        copy.start()

    barrier = pltpu.get_barrier_semaphore()
    greeted = jnp.int32(0)
    for n in range(1, 16):
        other = (z * 4 + cx + n) % 16
        oz, ox = other // 4, other % 4
        next_to = jnp.logical_and(ox == cx, jnp.logical_or(oz == z + 1, oz == z - 1))
        moved = jnp.logical_and(oz * z == 0, jnp.maximum(oz, z) < 3)
        meet = jnp.logical_or(oz == z, jnp.logical_or(next_to, moved))
        greeted += jnp.where(meet, 1, 0)

        @pl.when(meet)
        def _():
            pl.semaphore_signal(barrier, inc=1, device_id=(dp, oz, ox), device_id_type=MESH)

    for copy, src, dst in zip(loads[:2], (k_raw, v_raw), (k_ref, v_ref)):
        copy.wait()
        dst[...] = jnp.swapaxes(src[...], 0, 1)
    pl.semaphore_wait(barrier, greeted)

    for h in (0, 1):
        for half in (0, 1):
            for d in (2, 3, 1):
                kv_send(h, half, d)
            if h == 0:
                z_each(h, half, 0, z_own)

    for h in (0, 1):
        for half in (0, 1):
            own_kv(h, half)
    loads[2].wait()
    for n in range(4):
        q_ref[8 * n:8 * n + 8] = jnp.swapaxes(q_raw[:, 8 * n:8 * n + 8], 0, 1)

    def send_q(h, half):
        for d in (2, 3, 1):
            q_send(h, half, d).start()

    @pl.when(first)
    def _():
        send_q(1, 1)

    send_q(0, 0)
    send_q(0, 1)
    send_q(1, 0)

    @pl.when(jnp.logical_not(first))
    def _():
        send_q(1, 1)

    for h in (0, 1):
        for half in (0, 1):
            own_q(h, half)

    def relay_own(h):
        for half in (0, 1):
            if h == 1:
                z_each(h, half, 0, z_own)
            for d in (1, 2, 3):
                kv_both(h, half, d).wait_recv()
                z_each(h, half, d, z_own)

    order = words(z, PUMP, 4)

    def z_fwd(h, b, way):
        ref = kvb.at[h, b]
        return remote(ref, ref, f_s.at[h, b], z_r.at[h, b], z_dev(way))

    def fwd_ways(h, b):
        from_up = jnp.logical_and(b > z, b < 7 - z)
        down = jnp.logical_and(from_up, jnp.logical_or(z > 1, jnp.logical_and(second, h == 0)))
        up = jnp.logical_or(jnp.logical_and(has_up, b < z), jnp.logical_and(second, b == 7))
        return up, down

    def pump(i, _):
        code = entry(order, i, 4)
        h, b = code // 8, code % 8
        ref = kvb.at[h, b]
        remote(ref, ref, f_s.at[h, b], z_r.at[h, b], (dp, z, partners[1])).wait_recv()
        up, down = fwd_ways(h, b)

        @pl.when(down)
        def _():
            z_fwd(h, b, 1).start()

        @pl.when(up)
        def _():
            z_fwd(h, b, 0).start()

        return 0

    def fwd_wait(i, _):
        code = entry(order, i, 4)
        h, b = code // 8, code % 8
        up, down = fwd_ways(h, b)

        @pl.when(jnp.logical_or(up, down))
        def _():
            ref = kvb.at[h, b]
            remote(ref, ref, f_s.at[h, b], z_r.at[h, b], (dp, z, partners[1])).wait_send()

        return 0

    def chain(items):
        def scores(it):
            tile, h, b, nk, _, _ = it
            return lax.dot_general(qb[tile], kvb[h, b, 0, :nk], (((1,), (1,)), ((), ())), preferred_element_type=jnp.float32)

        def value(pend):
            tile, h, b, nk, p, alpha = pend
            pv = jnp.dot(p, kvb[h, b, 1, :nk], preferred_element_type=jnp.float32)
            ab[tile] = pv if alpha is None else alpha * ab[tile] + pv

        s = scores(items[0])
        pend = None
        for n, it in enumerate(items):
            nxt = scores(items[n + 1]) if n + 1 < len(items) else None
            tile, h, b, nk, mask, begins = it
            if mask is not None:
                s = jnp.where(mask, s, NEG)
            m = jnp.max(s, axis=1, keepdims=True)
            if begins:
                m = jnp.broadcast_to(m, (256, HD))
                alpha = None
            else:
                old = mb[tile]
                m = jnp.maximum(old, m)
                alpha = jnp.exp2((old - m) * c)
            mb[tile] = m
            p = jnp.exp2((s - jnp.concatenate([m] * (nk // HD), axis=1)) * c)
            tot = p[:, :HD]
            for j in range(1, nk // HD):
                tot = tot + p[:, j * HD:(j + 1) * HD]
            lb[tile] = tot if begins else alpha * lb[tile] + tot
            if pend is not None:
                value(pend)
            pend = (tile, h, b, nk, p.astype(jnp.bfloat16), alpha)
            s = nxt
        value(pend)

    def full(parts):
        chain([(g * 4 + t, h, b, B, None, False) for g, h, b in parts for t in range(4)])

    def diag(g, h, b, lower, begins):
        items = []
        for t, low in enumerate(lower):
            nk = 512 if low else 256
            row = lax.broadcasted_iota(jnp.int32, (256, nk), 0) + (256 if low else 0)
            mask = lax.broadcasted_iota(jnp.int32, (256, nk), 1) <= row
            items.append((g * 4 + t, h, b, nk, mask, begins))
        chain(items)

    def o_own(h, half):
        return pltpu.make_async_copy(
            rows4(ob, h, half, cx),
            o_ref.at[pl.ds(8 * cx + 4 * h, 4), pl.ds(half * S, S)], oloc.at[h, half])

    for t in range(32, 36):
        mb[t] = jnp.full((256, HD), NEG, jnp.float32)
        lb[t] = jnp.zeros((256, HD), jnp.float32)
        ab[t] = jnp.zeros((256, HD), jnp.float32)
    relay_own(0)
    count = [len(p) for p in PROGRAM]
    ops = words(z, PROGRAM, 28)

    def run(i, at):
        code = entry(ops, i, 28)
        op, upto = code % 8, (code // 8) % 16
        parts = []
        for n in range(3):
            gc, b = (code // 128 ** (n + 1)) % 16, (code // (16 * 128 ** (n + 1))) % 8
            y = jnp.where(gc % 2 == 0, cx // 2, 1 - cx // 2)
            parts.append((jnp.where(gc == X, X, gc - gc % 2 + y), jnp.where(gc < 4, 0, 1), b))
        gc, b = (code // 128) % 16, (code // 2048) % 8
        half, other, extra = (gc // 2) % 2, gc % 2, gc == X
        y = jnp.where(other == 0, cx // 2, 1 - cx // 2)
        g, h, _ = parts[0]
        lax.fori_loop(at, upto, pump, 0)

        for n, name in ((1, FULL), (2, FULL2), (3, FULL3)):
            @pl.when(op == name)
            def _():
                full(parts[:n])

        @pl.when(op == DIAG)
        def _():
            lower = jnp.where(half == 0, y == 1, y == 0)

            @pl.when(extra)
            def _():
                diag(8, 1, 7, (True, True, False, False), False)

            @pl.when(jnp.logical_not(extra))
            def _():
                @pl.when(other == 0)
                def _():
                    q_both(h, half, 1).wait_recv()

                @pl.when(other == 1)
                def _():
                    q_both(h, half, 2).wait_recv()
                    q_both(h, half, 3).wait_recv()

                @pl.when(lower)
                def _():
                    diag(g, h, b, (True,) * 4, True)

                @pl.when(jnp.logical_not(lower))
                def _():
                    diag(g, h, b, (False,) * 4, True)

        @pl.when(op == FIN)
        def _():
            for t in range(4):
                tile = g * 4 + t
                ob[tile] = (ab[tile] / jnp.sum(lb[tile], axis=1, keepdims=True)).astype(jnp.bfloat16)

            @pl.when(extra)
            def _():
                for d in (2, 3, 1, 0):
                    xo_send(d).start()

            @pl.when(jnp.logical_not(extra))
            def _():
                @pl.when(other == 0)
                def _():
                    o_send(h, half, 1).start()
                    o_own(h, half).start()

                @pl.when(other == 1)
                def _():
                    o_send(h, half, 2).start()
                    o_send(h, half, 3).start()

        @pl.when(op == OTHER)
        def _():
            @pl.when(b == 0)
            def _():
                relay_own(1)

            @pl.when(b == 1)
            def _():
                for d in (1, 2, 3):
                    q_both(1, 1, d).wait_recv()
                for n in (1,):
                    x_send(n)

            @pl.when(b == 2)
            def _():
                for d in range(4):
                    z_own(1, 1, d, 0)

                @pl.when(first)
                def _():
                    x_send(0)

            @pl.when(b == 3)
            def _():
                x_both(0).wait_recv()

        return upto

    lax.fori_loop(0, pick(z, count), run, jnp.int32(0))

    lax.fori_loop(0, pick(z, [len(p) for p in PUMP]), fwd_wait, 0)

    def z_wait(h, half, d, way):
        z_piece(h, half, d, way).wait_send()

    for h in (0, 1):
        for half in (0, 1):
            for d in (1, 2, 3):
                kv_both(h, half, d).wait_send()
                q_send(h, half, d).wait_send()
            for d in range(4):
                z_each(h, half, d, z_wait)
                if (h, half) == (1, 1):
                    @pl.when(z < 2)
                    def _():
                        z_wait(h, half, d, 0)

            def o_wait():
                o_own(h, half).wait()
                for d in (1, 2, 3):
                    o_send(h, half, d).wait_send()
                    o_recv(h, half, d).wait_recv()

            if (h, half) == (1, 1):
                pl.when(jnp.logical_not(first))(o_wait)
            else:
                o_wait()

    @pl.when(first)
    def _():
        for n in (0, 1):
            x_both(n).wait_send()
            for d in range(4):
                xo_recv(n, d).wait_recv()

    @pl.when(has_x)
    def _():
        for d in range(4):
            xo_send(d).wait_send()


PARTS = 8


def by_rows(x_ref, o_ref, x_in, out, in_sem, out_sem):
    rows = 256 // PARTS

    def fetch(n):
        at = pl.ds(n * rows, rows)
        return pltpu.make_async_copy(x_ref.at[:, at], x_in.at[n], in_sem.at[n])

    def put(n):
        at = pl.ds(n * rows, rows)
        return pltpu.make_async_copy(out.at[at], o_ref.at[at], out_sem.at[n])

    for n in range(PARTS):
        fetch(n).start()
    for n in range(PARTS):
        fetch(n).wait()
        for g in range(4):
            out[n * rows:(n + 1) * rows, 8 * g:8 * g + 8] = jnp.swapaxes(x_in[n, 8 * g:8 * g + 8], 0, 1)
        put(n).start()
    for n in range(PARTS):
        put(n).wait()


def solution(mesh):
    spec = P(("dp", "cy", "cx"))

    def local(q, k, v):
        dma = pltpu.SemaphoreType.DMA
        out = pl.pallas_call(
            kernel,
            out_shape=jax.ShapeDtypeStruct((32, 256, HD), jnp.bfloat16),
            in_specs=[pl.BlockSpec(memory_space=pl.ANY)] * 3,
            out_specs=pl.BlockSpec(memory_space=pl.ANY),
            scratch_shapes=[
                pltpu.VMEM((256, 32, HD), jnp.bfloat16),
                pltpu.VMEM((256, 8, HD), jnp.bfloat16),
                pltpu.VMEM((256, 8, HD), jnp.bfloat16),
                pltpu.VMEM((32, 256, HD), jnp.bfloat16),
                pltpu.VMEM((8, 256, HD), jnp.bfloat16),
                pltpu.VMEM((8, 256, HD), jnp.bfloat16),
                pltpu.VMEM((36, 256, HD), jnp.bfloat16),
                pltpu.VMEM((2, 8, 2, B, HD), jnp.bfloat16),
                pltpu.VMEM((36, 256, HD), jnp.bfloat16),
                pltpu.VMEM((36, 256, HD), jnp.float32),
                pltpu.VMEM((36, 256, HD), jnp.float32),
                pltpu.VMEM((36, 256, HD), jnp.float32),
                dma((2, 2, 3)), dma((2, 2, 3)),
                dma((2, 2, 3)), dma((2, 2, 3)),
                dma((2, 2, 4, 2)), dma((2, 8)), dma((2, 8)),
                dma((2, 2, 3)), dma((2, 2, 3)),
                dma((2,)), dma((1,)), dma((4,)), dma((2, 4)),
                dma((3,)), dma((2, 2)),
            ],
            compiler_params=pltpu.CompilerParams(
                collective_id=0, has_side_effects=True, vmem_limit_bytes=60 * 1024 * 1024),
        )(q, k, v)
        return pl.pallas_call(
            by_rows,
            out_shape=jax.ShapeDtypeStruct((256, 32, HD), jnp.bfloat16),
            in_specs=[pl.BlockSpec(memory_space=pl.ANY)],
            out_specs=pl.BlockSpec(memory_space=pl.ANY),
            scratch_shapes=[
                pltpu.VMEM((PARTS, 32, 256 // PARTS, HD), jnp.bfloat16),
                pltpu.VMEM((256, 32, HD), jnp.bfloat16),
                dma((PARTS,)), dma((PARTS,)),
            ],
            compiler_params=pltpu.CompilerParams(vmem_limit_bytes=60 * 1024 * 1024),
        )(out)

    return jax.shard_map(local, mesh=mesh, in_specs=(spec, spec, spec), out_specs=spec, check_vma=False)
```

```python
import jax
import jax.numpy as jnp
from jax import lax
from jax.experimental import pallas as pl
from jax.experimental.pallas import tpu as pltpu
from jax.sharding import PartitionSpec as P

MESH = pl.DeviceIdType.MESH
NEG = -1.0e30
LOG2E = 1.4426950408889634
B = 512
S = 128
HD = 128

PUMP = (
    (0x435261,),
    (0xcbdfa483520,),
    (0xef8c9b0431,),
    (0x890a12,),
)
FULL, DIAG, FIN, OTHER, FULL2, FULL3 = range(6)
X = 8
PROGRAM = (
    (0x90800001000003901, 0x13000000a0000009, 0x21200002110003110, 0x1118000101b000081b, 0xa200000a10002920,
     0x8c9ac00039a90001928, 0x10e134000f1ac014d9ac, 0x2b100001b20000132, 0x2b2,),
    (0x1200000080000801, 0x91000881140003111, 0x29180000a19000001b, 0x8a10000b180003319, 0x1822c00000aa00c80a4,
     0x8c1b400031b1000022a, 0x1ba004e9b4010d9b4, 0x1420001043009a13c, 0x2ca00002c00000ac1, 0x184b009c3cc00033c9,
     0x1a1c540062c4c00a044c, 0x11e45c015dbd40003c51, 0x3da00d8bdc000045a, 0x35a015a35c,),
    (0x291100008080001001, 0x1b000111000c8914, 0x13180002b190002118, 0x12200000220008024, 0xd8b3400440a400010a1,
     0x4c1b400029b100000b2, 0x12b9008e1bc00ce33c, 0x182c400001ba0000ab8, 0x2bc1000034200002c2, 0x184b011dbc4005c3c4,
     0x3c490121c4c006044c, 0x452009f454016144c, 0x50254000125100003d2, 0x252,),
    (0x210900010080001801, 0x2309000000b00c910c, 0x488140001a090001b08, 0x9131c00848940001891, 0x1998008c99c0002199,
     0x2200000a200000a4, 0x50b2c00001a200081a4, 0x9cbac00023a9000012a, 0x94aac0001aa90001ba8, 0x33200003b200183b4,
     0x2b200002320014234,),
)
TAKEN = (6, 11, 10, 6)
STEPS = (25, 41, 40, 33)
BOTH = (0, 1)
OTHERS = (1, 2, 3)
FAR_FIRST = (2, 3, 1)


def unpack(rows, bits, count):
    per = 84 // bits
    return [[rows[i // per] >> bits * (i % per) & (1 << bits) - 1 for i in range(n)] for rows, n in zip(rows, count)]


def pick(z, values):
    out = jnp.int32(values[0])
    for i in range(1, len(values)):
        out = jnp.where(z == i, jnp.int32(values[i]), out)
    return out


def words(z, seqs, bits):
    per = 31 // bits
    n = max(len(q) for q in seqs)
    return [pick(z, [sum(x << (bits * i) for i, x in enumerate(q[w:w + per])) for q in seqs])
            for w in range(0, n, per)]


def entry(table, i, bits):
    per = 31 // bits
    word = table[0]
    for w in range(1, len(table)):
        word = jnp.where(i >= per * w, table[w], word)
    return lax.shift_right_logical(word, bits * (i % per)) & ((1 << bits) - 1)


def kernel(q_in, k_in, v_in, o_ref, q_raw, k_raw, v_raw, q_ref, k_ref, v_ref, qb, kvb, ob, mb, lb, ab,
           kv_s, kv_r, q_s, q_r, z_s, z_r, f_s, o_s, o_r, x_s, x_r, xo_s, xo_r, loc, oloc):
    dp = lax.axis_index("dp")
    z = lax.axis_index("cy")
    cx = lax.axis_index("cx")
    c = (HD ** -0.5) * LOG2E
    partners = (cx, cx + 1 - 2 * (cx % 2), (cx + 2) % 4, 3 - cx)
    first, second = z == 0, z == 1
    has_dn, has_up = z > 0, z < 3
    has_x = jnp.logical_and(z >= 1, z <= 2)

    def span_at(half, who):
        return (who if half == 0 else 3 - who) * S

    def blk(half):
        return z if half == 0 else 7 - z

    def remote(src, dst, ssem, rsem, dev):
        return pltpu.make_async_remote_copy(src, dst, ssem, rsem, device_id=dev, device_id_type=MESH)

    def kv_piece(h, half, who):
        return kvb.at[h, blk(half), :, pl.ds(span_at(half, who), S)]

    def kv_send(h, half, d):
        t = partners[d]
        for ref, n in ((k_ref, 0), (v_ref, 1)):
            remote(ref.at[2 * t + h, pl.ds(half * S, S)], kvb.at[h, blk(half), n, pl.ds(span_at(half, cx), S)],
                   kv_s.at[h, half, d - 1], kv_r.at[h, half, d - 1], (dp, z, t)).start()

    def kv_both(h, half, d):
        ref = kv_piece(h, half, partners[d])
        return remote(ref, ref, kv_s.at[h, half, d - 1], kv_r.at[h, half, d - 1], (dp, z, partners[d]))

    def rows4(ref, h, half, who):
        at = jnp.where(half == 0, who % 2, 1 - who % 2) * S
        return ref.at[pl.ds(((h * 2 + half) * 2 + who // 2) * 4, 4), pl.ds(at, S)]

    def q_piece(h, half, who):
        return rows4(qb, h, half, who)

    def q_send(h, half, d):
        t = partners[d]
        return remote(q_ref.at[pl.ds(8 * t + 4 * h, 4), pl.ds(half * S, S)], q_piece(h, half, cx),
                      q_s.at[h, half, d - 1], q_r.at[h, half, d - 1], (dp, z, t))

    def q_both(h, half, d):
        ref = q_piece(h, half, partners[d])
        return remote(ref, ref, q_s.at[h, half, d - 1], q_r.at[h, half, d - 1], (dp, z, partners[d]))

    def o_send(h, half, d):
        t = partners[d]
        return remote(rows4(ob, h, half, t),
                      o_ref.at[pl.ds(8 * cx + 4 * h, 4), pl.ds(half * S, S)],
                      o_s.at[h, half, d - 1], o_r.at[h, half, d - 1], (dp, z, t))

    def o_recv(h, half, d):
        t = partners[d]
        ref = o_ref.at[pl.ds(8 * t + 4 * h, 4), pl.ds(half * S, S)]
        return remote(ref, ref, o_s.at[h, half, d - 1], o_r.at[h, half, d - 1], (dp, z, t))

    def x_send(n):
        for y in BOTH:
            remote(qb.at[pl.ds((6 + y) * 4 + 2 * n, 2)], qb.at[pl.ds(32 + 2 * y, 2)],
                   x_s.at[n], x_r.at[0], (dp, n + 1, cx)).start()

    def x_both(n):
        ref = qb.at[pl.ds(32, 4)]
        return remote(ref, ref, x_s.at[n], x_r.at[0], (dp, 0, cx))

    def xo_send(d):
        t = partners[d]
        return remote(ob.at[pl.ds(32 + 2 * (t // 2), 2), pl.ds((1 - t % 2) * S, S)],
                      o_ref.at[pl.ds(8 * cx + 2 + 2 * z, 2), pl.ds(S, S)],
                      xo_s.at[d], xo_r.at[z - 1, d], (dp, 0, t))

    def xo_recv(n, d):
        ref = o_ref.at[pl.ds(8 * partners[d] + 4 + 2 * n, 2), pl.ds(S, S)]
        return remote(ref, ref, xo_s.at[d], xo_r.at[n, d], (dp, n + 1, partners[d]))

    def z_dev(way):
        return (dp, z + 1 if way == 0 else z - 1, cx)

    def z_own(h, half, d, way):
        b = blk(half)
        if d == 0:
            for ref, n in ((k_ref, 0), (v_ref, 1)):
                remote(ref.at[2 * cx + h, pl.ds(half * S, S)], kvb.at[h, b, n, pl.ds(span_at(half, cx), S)],
                       z_s.at[h, half, d, way], z_r.at[h, b], z_dev(way)).start()
        else:
            z_piece(h, half, d, way).start()

    def z_piece(h, half, d, way):
        ref = kv_piece(h, half, partners[d])
        return remote(ref, ref, z_s.at[h, half, d, way], z_r.at[h, blk(half)], z_dev(way))

    def z_cond(h, half, way):
        if way == 0:
            return has_up if half == 0 else None
        return has_dn if h == 0 else z > 1

    def z_each(h, half, d, do):
        for way in BOTH:
            cond = z_cond(h, half, way)
            if cond is not None:
                @pl.when(cond)
                def _():
                    do(h, half, d, way)

    def own_kv(h, half):
        for ref, n in ((k_ref, 0), (v_ref, 1)):
            kvb[h, blk(half), n, pl.ds(span_at(half, cx), S)] = ref[2 * cx + h, half * S:(half + 1) * S]

    def own_q(h, half):
        at = (cx % 2 if half == 0 else 1 - cx % 2) * S
        for t in range(4):
            qb[((h * 2 + half) * 2 + cx // 2) * 4 + t, pl.ds(at, S)] = q_ref[8 * cx + 4 * h + t, half * S:(half + 1) * S]

    loads = [pltpu.make_async_copy(src, dst, loc.at[n])
             for n, (src, dst) in enumerate(((k_in, k_raw), (v_in, v_raw), (q_in, q_raw)))]
    for copy in loads:
        copy.start()

    barrier = pltpu.get_barrier_semaphore()
    greeted = jnp.int32(0)
    for n in range(1, 16):
        other = (z * 4 + cx + n) % 16
        oz, ox = other // 4, other % 4
        next_to = jnp.logical_and(ox == cx, jnp.logical_or(oz == z + 1, oz == z - 1))
        moved = jnp.logical_and(oz * z == 0, jnp.maximum(oz, z) < 3)
        meet = jnp.logical_or(oz == z, jnp.logical_or(next_to, moved))
        greeted += jnp.where(meet, 1, 0)

        @pl.when(meet)
        def _():
            pl.semaphore_signal(barrier, inc=1, device_id=(dp, oz, ox), device_id_type=MESH)

    for copy, src, dst in zip(loads[:2], (k_raw, v_raw), (k_ref, v_ref)):
        copy.wait()
        dst[...] = jnp.swapaxes(src[...], 0, 1)
    pl.semaphore_wait(barrier, greeted)

    for h in BOTH:
        for half in BOTH:
            for d in FAR_FIRST:
                kv_send(h, half, d)
            if h == 0:
                z_each(h, half, 0, z_own)

    for h in BOTH:
        for half in BOTH:
            own_kv(h, half)
    loads[2].wait()
    for n in range(4):
        q_ref[8 * n:8 * n + 8] = jnp.swapaxes(q_raw[:, 8 * n:8 * n + 8], 0, 1)

    def send_q(h, half):
        for d in FAR_FIRST:
            q_send(h, half, d).start()

    @pl.when(first)
    def _():
        send_q(1, 1)

    send_q(0, 0)
    send_q(0, 1)
    send_q(1, 0)

    @pl.when(jnp.logical_not(first))
    def _():
        send_q(1, 1)

    for h in BOTH:
        for half in BOTH:
            own_q(h, half)

    def relay_own(h):
        for half in BOTH:
            if h == 1:
                z_each(h, half, 0, z_own)
            for d in OTHERS:
                kv_both(h, half, d).wait_recv()
                z_each(h, half, d, z_own)

    order = words(z, unpack(PUMP, 4, TAKEN), 4)

    def z_fwd(h, b, way):
        ref = kvb.at[h, b]
        return remote(ref, ref, f_s.at[h, b], z_r.at[h, b], z_dev(way))

    def fwd_ways(h, b):
        from_up = jnp.logical_and(b > z, b < 7 - z)
        down = jnp.logical_and(from_up, jnp.logical_or(z > 1, jnp.logical_and(second, h == 0)))
        up = jnp.logical_or(jnp.logical_and(has_up, b < z), jnp.logical_and(second, b == 7))
        return up, down

    def pump(i, _):
        code = entry(order, i, 4)
        h, b = code // 8, code % 8
        ref = kvb.at[h, b]
        remote(ref, ref, f_s.at[h, b], z_r.at[h, b], (dp, z, partners[1])).wait_recv()
        up, down = fwd_ways(h, b)

        @pl.when(down)
        def _():
            z_fwd(h, b, 1).start()

        @pl.when(up)
        def _():
            z_fwd(h, b, 0).start()

        return 0

    def fwd_wait(i, _):
        code = entry(order, i, 4)
        h, b = code // 8, code % 8
        up, down = fwd_ways(h, b)

        @pl.when(jnp.logical_or(up, down))
        def _():
            ref = kvb.at[h, b]
            remote(ref, ref, f_s.at[h, b], z_r.at[h, b], (dp, z, partners[1])).wait_send()

        return 0

    def chain(items):
        def scores(it):
            tile, h, b, nk, _, _ = it
            return lax.dot_general(qb[tile], kvb[h, b, 0, :nk], (((1,), (1,)), ((), ())), preferred_element_type=jnp.float32)

        def value(pend):
            tile, h, b, nk, p, alpha = pend
            pv = jnp.dot(p, kvb[h, b, 1, :nk], preferred_element_type=jnp.float32)
            ab[tile] = pv if alpha is None else alpha * ab[tile] + pv

        s = scores(items[0])
        pend = None
        for n, it in enumerate(items):
            nxt = scores(items[n + 1]) if n + 1 < len(items) else None
            tile, h, b, nk, mask, begins = it
            if mask is not None:
                s = jnp.where(mask, s, NEG)
            m = jnp.max(s, axis=1, keepdims=True)
            if begins:
                m = jnp.broadcast_to(m, (256, HD))
                alpha = None
            else:
                old = mb[tile]
                m = jnp.maximum(old, m)
                alpha = jnp.exp2((old - m) * c)
            mb[tile] = m
            p = jnp.exp2((s - jnp.concatenate([m] * (nk // HD), axis=1)) * c)
            tot = p[:, :HD]
            for j in range(1, nk // HD):
                tot = tot + p[:, j * HD:(j + 1) * HD]
            lb[tile] = tot if begins else alpha * lb[tile] + tot
            if pend is not None:
                value(pend)
            pend = (tile, h, b, nk, p.astype(jnp.bfloat16), alpha)
            s = nxt
        value(pend)

    def full(parts):
        chain([(g * 4 + t, h, b, B, None, False) for g, h, b in parts for t in range(4)])

    def diag(g, h, b, lower, begins):
        items = []
        for t, low in enumerate(lower):
            nk = 512 if low else 256
            row = lax.broadcasted_iota(jnp.int32, (256, nk), 0) + (256 if low else 0)
            mask = lax.broadcasted_iota(jnp.int32, (256, nk), 1) <= row
            items.append((g * 4 + t, h, b, nk, mask, begins))
        chain(items)

    def o_own(h, half):
        return pltpu.make_async_copy(
            rows4(ob, h, half, cx),
            o_ref.at[pl.ds(8 * cx + 4 * h, 4), pl.ds(half * S, S)], oloc.at[h, half])

    for t in range(32, 36):
        mb[t] = jnp.full((256, HD), NEG, jnp.float32)
        lb[t] = jnp.zeros((256, HD), jnp.float32)
        ab[t] = jnp.zeros((256, HD), jnp.float32)
    relay_own(0)
    ops = words(z, unpack(PROGRAM, 28, STEPS), 28)

    def run(i, at):
        code = entry(ops, i, 28)
        op, upto = code % 8, (code // 8) % 16
        parts = []
        for n in range(3):
            gc, b = (code // 128 ** (n + 1)) % 16, (code // (16 * 128 ** (n + 1))) % 8
            y = jnp.where(gc % 2 == 0, cx // 2, 1 - cx // 2)
            parts.append((jnp.where(gc == X, X, gc - gc % 2 + y), jnp.where(gc < 4, 0, 1), b))
        gc, b = (code // 128) % 16, (code // 2048) % 8
        half, other, extra = (gc // 2) % 2, gc % 2, gc == X
        y = jnp.where(other == 0, cx // 2, 1 - cx // 2)
        g, h, _ = parts[0]
        lax.fori_loop(at, upto, pump, 0)

        for n, name in ((1, FULL), (2, FULL2), (3, FULL3)):
            @pl.when(op == name)
            def _():
                full(parts[:n])

        @pl.when(op == DIAG)
        def _():
            lower = jnp.where(half == 0, y == 1, y == 0)

            @pl.when(extra)
            def _():
                diag(8, 1, 7, (True, True, False, False), False)

            @pl.when(jnp.logical_not(extra))
            def _():
                @pl.when(other == 0)
                def _():
                    q_both(h, half, 1).wait_recv()

                @pl.when(other == 1)
                def _():
                    q_both(h, half, 2).wait_recv()
                    q_both(h, half, 3).wait_recv()

                @pl.when(lower)
                def _():
                    diag(g, h, b, (True,) * 4, True)

                @pl.when(jnp.logical_not(lower))
                def _():
                    diag(g, h, b, (False,) * 4, True)

        @pl.when(op == FIN)
        def _():
            for t in range(4):
                tile = g * 4 + t
                ob[tile] = (ab[tile] / jnp.sum(lb[tile], axis=1, keepdims=True)).astype(jnp.bfloat16)

            @pl.when(extra)
            def _():
                for d in (2, 3, 1, 0):
                    xo_send(d).start()

            @pl.when(jnp.logical_not(extra))
            def _():
                @pl.when(other == 0)
                def _():
                    o_send(h, half, 1).start()
                    o_own(h, half).start()

                @pl.when(other == 1)
                def _():
                    o_send(h, half, 2).start()
                    o_send(h, half, 3).start()

        @pl.when(op == OTHER)
        def _():
            @pl.when(b == 0)
            def _():
                relay_own(1)

            @pl.when(b == 1)
            def _():
                for d in OTHERS:
                    q_both(1, 1, d).wait_recv()
                for n in (1,):
                    x_send(n)

            @pl.when(b == 2)
            def _():
                for d in range(4):
                    z_own(1, 1, d, 0)

                @pl.when(first)
                def _():
                    x_send(0)

            @pl.when(b == 3)
            def _():
                x_both(0).wait_recv()

        return upto

    lax.fori_loop(0, pick(z, STEPS), run, jnp.int32(0))

    lax.fori_loop(0, pick(z, TAKEN), fwd_wait, 0)

    def z_wait(h, half, d, way):
        z_piece(h, half, d, way).wait_send()

    for h in BOTH:
        for half in BOTH:
            for d in OTHERS:
                kv_both(h, half, d).wait_send()
                q_send(h, half, d).wait_send()
            for d in range(4):
                z_each(h, half, d, z_wait)
                if (h, half) == (1, 1):
                    @pl.when(z < 2)
                    def _():
                        z_wait(h, half, d, 0)

            def o_wait():
                o_own(h, half).wait()
                for d in OTHERS:
                    o_send(h, half, d).wait_send()
                    o_recv(h, half, d).wait_recv()

            if (h, half) == (1, 1):
                pl.when(jnp.logical_not(first))(o_wait)
            else:
                o_wait()

    @pl.when(first)
    def _():
        for n in BOTH:
            x_both(n).wait_send()
            for d in range(4):
                xo_recv(n, d).wait_recv()

    @pl.when(has_x)
    def _():
        for d in range(4):
            xo_send(d).wait_send()


PARTS = 8


def by_rows(x_ref, o_ref, x_in, out, in_sem, out_sem):
    rows = 256 // PARTS

    def fetch(n):
        at = pl.ds(n * rows, rows)
        return pltpu.make_async_copy(x_ref.at[:, at], x_in.at[n], in_sem.at[n])

    def put(n):
        at = pl.ds(n * rows, rows)
        return pltpu.make_async_copy(out.at[at], o_ref.at[at], out_sem.at[n])

    for n in range(PARTS):
        fetch(n).start()
    for n in range(PARTS):
        fetch(n).wait()
        for g in range(4):
            out[n * rows:(n + 1) * rows, 8 * g:8 * g + 8] = jnp.swapaxes(x_in[n, 8 * g:8 * g + 8], 0, 1)
        put(n).start()
    for n in range(PARTS):
        put(n).wait()


def solution(mesh):
    spec = P(("dp", "cy", "cx"))

    def local(q, k, v):
        dma = pltpu.SemaphoreType.DMA
        out = pl.pallas_call(
            kernel,
            out_shape=jax.ShapeDtypeStruct((32, 256, HD), jnp.bfloat16),
            in_specs=[pl.BlockSpec(memory_space=pl.ANY)] * 3,
            out_specs=pl.BlockSpec(memory_space=pl.ANY),
            scratch_shapes=[
                pltpu.VMEM((256, 32, HD), jnp.bfloat16),
                pltpu.VMEM((256, 8, HD), jnp.bfloat16),
                pltpu.VMEM((256, 8, HD), jnp.bfloat16),
                pltpu.VMEM((32, 256, HD), jnp.bfloat16),
                pltpu.VMEM((8, 256, HD), jnp.bfloat16),
                pltpu.VMEM((8, 256, HD), jnp.bfloat16),
                pltpu.VMEM((36, 256, HD), jnp.bfloat16),
                pltpu.VMEM((2, 8, 2, B, HD), jnp.bfloat16),
                pltpu.VMEM((36, 256, HD), jnp.bfloat16),
                pltpu.VMEM((36, 256, HD), jnp.float32),
                pltpu.VMEM((36, 256, HD), jnp.float32),
                pltpu.VMEM((36, 256, HD), jnp.float32),
                dma((2, 2, 3)), dma((2, 2, 3)),
                dma((2, 2, 3)), dma((2, 2, 3)),
                dma((2, 2, 4, 2)), dma((2, 8)), dma((2, 8)),
                dma((2, 2, 3)), dma((2, 2, 3)),
                dma((2,)), dma((1,)), dma((4,)), dma((2, 4)),
                dma((3,)), dma((2, 2)),
            ],
            compiler_params=pltpu.CompilerParams(
                collective_id=0, has_side_effects=True, vmem_limit_bytes=60 * 1024 * 1024),
        )(q, k, v)
        return pl.pallas_call(
            by_rows,
            out_shape=jax.ShapeDtypeStruct((256, 32, HD), jnp.bfloat16),
            in_specs=[pl.BlockSpec(memory_space=pl.ANY)],
            out_specs=pl.BlockSpec(memory_space=pl.ANY),
            scratch_shapes=[
                pltpu.VMEM((PARTS, 32, 256 // PARTS, HD), jnp.bfloat16),
                pltpu.VMEM((256, 32, HD), jnp.bfloat16),
                dma((PARTS,)), dma((PARTS,)),
            ],
            compiler_params=pltpu.CompilerParams(vmem_limit_bytes=60 * 1024 * 1024),
        )(out)

    return jax.shard_map(local, mesh=mesh, in_specs=(spec, spec, spec), out_specs=spec, check_vma=False)
```

```python
import jax
import jax.numpy as jnp
from jax import lax
from jax.experimental import pallas as pl
from jax.experimental.pallas import tpu as pltpu
from jax.sharding import PartitionSpec as P

MESH = pl.DeviceIdType.MESH
NEG = -1.0e30
LOG2E = 1.4426950408889634
B = 512
S = 128
HD = 128

PUMP = (
    (0x435261,),
    (0xcbdfa483520,),
    (0xef8c9b0431,),
    (0x890a12,),
)
FULL, DIAG, FIN, OTHER, FULL2, FULL3 = range(6)
X = 8
PROGRAM = (
    (0x90800001000003901, 0x13000000a0000009, 0x21200002110003110, 0x1118000101b000081b, 0xa200000a10002920,
     0x8c9ac00039a90001928, 0x10e134000f1ac014d9ac, 0x2b100001b20000132, 0x2b2,),
    (0x1200000080000801, 0x91000881140003111, 0x29180000a19000001b, 0x8a10000b180003319, 0x1822c00000aa00c80a4,
     0x8c1b400031b1000022a, 0x1ba004e9b4010d9b4, 0x1420001043009a13c, 0x2ca00002c00000ac1, 0x184b009c3cc00033c9,
     0x1a1c540062c4c00a044c, 0x11e45c015dbd40003c51, 0x3da00d8bdc000045a, 0x35a015a35c,),
    (0x291100008080001001, 0x1b000111000c8914, 0x13180002b190002118, 0x12200000220008024, 0xd8b3400440a400010a1,
     0x4c1b400029b100000b2, 0x12b9008e1bc00ce33c, 0x182c400001ba0000ab8, 0x2bc1000034200002c2, 0x184b011dbc4005c3c4,
     0x3c490121c4c006044c, 0x452009f454016144c, 0x50254000125100003d2, 0x252,),
    (0x210900010080001801, 0x2309000000b00c910c, 0x488140001a090001b08, 0x9131c00848940001891, 0x1998008c99c0002199,
     0x2200000a200000a4, 0x50b2c00001a200081a4, 0x9cbac00023a9000012a, 0x94aac0001aa90001ba8, 0x33200003b200183b4,
     0x2b200002320014234,),
)
TAKEN = (6, 11, 10, 6)
STEPS = (25, 41, 40, 33)
BOTH = (0, 1)
OTHERS = (1, 2, 3)
FAR_FIRST = (2, 3, 1)


def unpack(rows, bits, count):
    per = 84 // bits
    return [[rows[i // per] >> bits * (i % per) & (1 << bits) - 1 for i in range(n)] for rows, n in zip(rows, count)]


def pick(z, values):
    out = jnp.int32(values[0])
    for i in range(1, len(values)):
        out = jnp.where(z == i, jnp.int32(values[i]), out)
    return out


def words(z, seqs, bits):
    per = 31 // bits
    n = max(len(q) for q in seqs)
    return [pick(z, [sum(x << (bits * i) for i, x in enumerate(q[w:w + per])) for q in seqs])
            for w in range(0, n, per)]


def entry(table, i, bits):
    per = 31 // bits
    word = table[0]
    for w in range(1, len(table)):
        word = jnp.where(i >= per * w, table[w], word)
    return lax.shift_right_logical(word, bits * (i % per)) & ((1 << bits) - 1)


def kernel(q_in, k_in, v_in, o_ref, q_raw, k_raw, v_raw, q_ref, k_ref, v_ref, qb, kvb, ob, mb, lb, ab,
           kv_s, kv_r, q_s, q_r, z_s, z_r, f_s, o_s, o_r, x_s, x_r, xo_s, xo_r, loc, oloc):
    dp = lax.axis_index("dp")
    z = lax.axis_index("cy")
    cx = lax.axis_index("cx")
    c = (HD ** -0.5) * LOG2E
    partners = (cx, cx + 1 - 2 * (cx % 2), (cx + 2) % 4, 3 - cx)
    first, second = z == 0, z == 1
    has_dn, has_up = z > 0, z < 3
    has_x = jnp.logical_and(z >= 1, z <= 2)

    def span_at(half, who):
        return (who if half == 0 else 3 - who) * S

    def blk(half):
        return z if half == 0 else 7 - z

    def remote(src, dst, ssem, rsem, dev):
        return pltpu.make_async_remote_copy(src, dst, ssem, rsem, device_id=dev, device_id_type=MESH)

    def kv_piece(h, half, who):
        return kvb.at[h, blk(half), :, pl.ds(span_at(half, who), S)]

    def kv_send(h, half, d):
        t = partners[d]
        for ref, n in ((k_ref, 0), (v_ref, 1)):
            remote(ref.at[2 * t + h, pl.ds(half * S, S)], kvb.at[h, blk(half), n, pl.ds(span_at(half, cx), S)],
                   kv_s.at[h, half, d - 1], kv_r.at[h, half, d - 1], (dp, z, t)).start()

    def kv_both(h, half, d):
        ref = kv_piece(h, half, partners[d])
        return remote(ref, ref, kv_s.at[h, half, d - 1], kv_r.at[h, half, d - 1], (dp, z, partners[d]))

    def rows4(ref, h, half, who):
        at = jnp.where(half == 0, who % 2, 1 - who % 2) * S
        return ref.at[pl.ds(((h * 2 + half) * 2 + who // 2) * 4, 4), pl.ds(at, S)]

    def q_piece(h, half, who):
        return rows4(qb, h, half, who)

    def q_send(h, half, d):
        t = partners[d]
        return remote(q_ref.at[pl.ds(8 * t + 4 * h, 4), pl.ds(half * S, S)], q_piece(h, half, cx),
                      q_s.at[h, half, d - 1], q_r.at[h, half, d - 1], (dp, z, t))

    def q_both(h, half, d):
        ref = q_piece(h, half, partners[d])
        return remote(ref, ref, q_s.at[h, half, d - 1], q_r.at[h, half, d - 1], (dp, z, partners[d]))

    def o_send(h, half, d):
        t = partners[d]
        return remote(rows4(ob, h, half, t),
                      o_ref.at[pl.ds(8 * cx + 4 * h, 4), pl.ds(half * S, S)],
                      o_s.at[h, half, d - 1], o_r.at[h, half, d - 1], (dp, z, t))

    def o_recv(h, half, d):
        t = partners[d]
        ref = o_ref.at[pl.ds(8 * t + 4 * h, 4), pl.ds(half * S, S)]
        return remote(ref, ref, o_s.at[h, half, d - 1], o_r.at[h, half, d - 1], (dp, z, t))

    def x_send(n):
        for y in BOTH:
            remote(qb.at[pl.ds((6 + y) * 4 + 2 * n, 2)], qb.at[pl.ds(32 + 2 * y, 2)],
                   x_s.at[n], x_r.at[0], (dp, n + 1, cx)).start()

    def x_both(n):
        ref = qb.at[pl.ds(32, 4)]
        return remote(ref, ref, x_s.at[n], x_r.at[0], (dp, 0, cx))

    def xo_send(d):
        t = partners[d]
        return remote(ob.at[pl.ds(32 + 2 * (t // 2), 2), pl.ds((1 - t % 2) * S, S)],
                      o_ref.at[pl.ds(8 * cx + 2 + 2 * z, 2), pl.ds(S, S)],
                      xo_s.at[d], xo_r.at[z - 1, d], (dp, 0, t))

    def xo_recv(n, d):
        ref = o_ref.at[pl.ds(8 * partners[d] + 4 + 2 * n, 2), pl.ds(S, S)]
        return remote(ref, ref, xo_s.at[d], xo_r.at[n, d], (dp, n + 1, partners[d]))

    def z_dev(way):
        return (dp, z + 1 if way == 0 else z - 1, cx)

    def z_own(h, half, d, way):
        b = blk(half)
        if d == 0:
            for ref, n in ((k_ref, 0), (v_ref, 1)):
                remote(ref.at[2 * cx + h, pl.ds(half * S, S)], kvb.at[h, b, n, pl.ds(span_at(half, cx), S)],
                       z_s.at[h, half, d, way], z_r.at[h, b], z_dev(way)).start()
        else:
            z_piece(h, half, d, way).start()

    def z_piece(h, half, d, way):
        ref = kv_piece(h, half, partners[d])
        return remote(ref, ref, z_s.at[h, half, d, way], z_r.at[h, blk(half)], z_dev(way))

    def z_cond(h, half, way):
        if way == 0:
            return has_up if half == 0 else None
        return has_dn if h == 0 else z > 1

    def z_each(h, half, d, do):
        for way in BOTH:
            cond = z_cond(h, half, way)
            if cond is not None:
                @pl.when(cond)
                def _():
                    do(h, half, d, way)

    def own_kv(h, half):
        for ref, n in ((k_ref, 0), (v_ref, 1)):
            kvb[h, blk(half), n, pl.ds(span_at(half, cx), S)] = ref[2 * cx + h, half * S:(half + 1) * S]

    def own_q(h, half):
        at = (cx % 2 if half == 0 else 1 - cx % 2) * S
        for t in range(4):
            qb[((h * 2 + half) * 2 + cx // 2) * 4 + t, pl.ds(at, S)] = q_ref[8 * cx + 4 * h + t, half * S:(half + 1) * S]

    loads = [pltpu.make_async_copy(src, dst, loc.at[n])
             for n, (src, dst) in enumerate(((k_in, k_raw), (v_in, v_raw), (q_in, q_raw)))]
    for copy in loads:
        copy.start()

    barrier = pltpu.get_barrier_semaphore()
    greeted = jnp.int32(0)
    for n in range(1, 16):
        other = (z * 4 + cx + n) % 16
        oz, ox = other // 4, other % 4
        next_to = jnp.logical_and(ox == cx, jnp.logical_or(oz == z + 1, oz == z - 1))
        moved = jnp.logical_and(oz * z == 0, jnp.maximum(oz, z) < 3)
        meet = jnp.logical_or(oz == z, jnp.logical_or(next_to, moved))
        greeted += jnp.where(meet, 1, 0)

        @pl.when(meet)
        def _():
            pl.semaphore_signal(barrier, inc=1, device_id=(dp, oz, ox), device_id_type=MESH)

    for copy, src, dst in zip(loads[:2], (k_raw, v_raw), (k_ref, v_ref)):
        copy.wait()
        dst[...] = jnp.swapaxes(src[...], 0, 1)
    pl.semaphore_wait(barrier, greeted)

    for h in BOTH:
        for half in BOTH:
            for d in FAR_FIRST:
                kv_send(h, half, d)
            if h == 0:
                z_each(h, half, 0, z_own)

    for h in BOTH:
        for half in BOTH:
            own_kv(h, half)
    loads[2].wait()
    for n in range(4):
        q_ref[8 * n:8 * n + 8] = jnp.swapaxes(q_raw[:, 8 * n:8 * n + 8], 0, 1)

    def send_q(h, half):
        for d in FAR_FIRST:
            q_send(h, half, d).start()

    @pl.when(first)
    def _():
        send_q(1, 1)

    send_q(0, 0)
    send_q(0, 1)
    send_q(1, 0)

    @pl.when(jnp.logical_not(first))
    def _():
        send_q(1, 1)

    for h in BOTH:
        for half in BOTH:
            own_q(h, half)

    def relay_own(h):
        for half in BOTH:
            if h == 1:
                z_each(h, half, 0, z_own)
            for d in OTHERS:
                kv_both(h, half, d).wait_recv()
                z_each(h, half, d, z_own)

    order = words(z, unpack(PUMP, 4, TAKEN), 4)

    def z_fwd(h, b, way):
        ref = kvb.at[h, b]
        return remote(ref, ref, f_s.at[h, b], z_r.at[h, b], z_dev(way))

    def fwd_ways(h, b):
        from_up = jnp.logical_and(b > z, b < 7 - z)
        down = jnp.logical_and(from_up, jnp.logical_or(z > 1, jnp.logical_and(second, h == 0)))
        up = jnp.logical_or(jnp.logical_and(has_up, b < z), jnp.logical_and(second, b == 7))
        return up, down

    def pump(i, _):
        code = entry(order, i, 4)
        h, b = code // 8, code % 8
        ref = kvb.at[h, b]
        remote(ref, ref, f_s.at[h, b], z_r.at[h, b], (dp, z, partners[1])).wait_recv()
        up, down = fwd_ways(h, b)

        @pl.when(down)
        def _():
            z_fwd(h, b, 1).start()

        @pl.when(up)
        def _():
            z_fwd(h, b, 0).start()

        return 0

    def fwd_wait(i, _):
        code = entry(order, i, 4)
        h, b = code // 8, code % 8
        up, down = fwd_ways(h, b)

        @pl.when(jnp.logical_or(up, down))
        def _():
            ref = kvb.at[h, b]
            remote(ref, ref, f_s.at[h, b], z_r.at[h, b], (dp, z, partners[1])).wait_send()

        return 0

    def chain(items):
        def scores(it):
            tile, h, b, nk, _, _ = it
            return lax.dot_general(qb[tile], kvb[h, b, 0, :nk], (((1,), (1,)), ((), ())), preferred_element_type=jnp.float32)

        def value(pend):
            tile, h, b, nk, p, alpha = pend
            pv = jnp.dot(p, kvb[h, b, 1, :nk], preferred_element_type=jnp.float32)
            ab[tile] = pv if alpha is None else alpha * ab[tile] + pv

        s = scores(items[0])
        pend = None
        for n, it in enumerate(items):
            nxt = scores(items[n + 1]) if n + 1 < len(items) else None
            tile, h, b, nk, mask, begins = it
            if mask is not None:
                s = jnp.where(mask, s, NEG)
            m = jnp.max(s, axis=1, keepdims=True)
            if begins:
                m = jnp.broadcast_to(m, (256, HD))
                alpha = None
            else:
                old = mb[tile]
                m = jnp.maximum(old, m)
                alpha = jnp.exp2((old - m) * c)
            mb[tile] = m
            p = jnp.exp2((s - jnp.concatenate([m] * (nk // HD), axis=1)) * c)
            tot = p[:, :HD]
            for j in range(1, nk // HD):
                tot = tot + p[:, j * HD:(j + 1) * HD]
            lb[tile] = tot if begins else alpha * lb[tile] + tot
            if pend is not None:
                value(pend)
            pend = (tile, h, b, nk, p.astype(jnp.bfloat16), alpha)
            s = nxt
        value(pend)

    def full(parts):
        chain([(g * 4 + t, h, b, B, None, False) for g, h, b in parts for t in range(4)])

    def diag(g, h, b, lower, begins):
        items = []
        for t, low in enumerate(lower):
            nk = 512 if low else 256
            row = lax.broadcasted_iota(jnp.int32, (256, nk), 0) + (256 if low else 0)
            mask = lax.broadcasted_iota(jnp.int32, (256, nk), 1) <= row
            items.append((g * 4 + t, h, b, nk, mask, begins))
        chain(items)

    def o_own(h, half):
        return pltpu.make_async_copy(
            rows4(ob, h, half, cx),
            o_ref.at[pl.ds(8 * cx + 4 * h, 4), pl.ds(half * S, S)], oloc.at[h, half])

    for t in range(32, 36):
        mb[t] = jnp.full((256, HD), NEG, jnp.float32)
        lb[t] = jnp.zeros((256, HD), jnp.float32)
        ab[t] = jnp.zeros((256, HD), jnp.float32)
    relay_own(0)
    ops = words(z, unpack(PROGRAM, 28, STEPS), 28)

    def run(i, at):
        code = entry(ops, i, 28)
        op, upto = code % 8, (code // 8) % 16
        parts = []
        for n in range(3):
            gc, b = (code // 128 ** (n + 1)) % 16, (code // (16 * 128 ** (n + 1))) % 8
            y = jnp.where(gc % 2 == 0, cx // 2, 1 - cx // 2)
            parts.append((jnp.where(gc == X, X, gc - gc % 2 + y), jnp.where(gc < 4, 0, 1), b))
        gc, b = (code // 128) % 16, (code // 2048) % 8
        half, other, extra = (gc // 2) % 2, gc % 2, gc == X
        y = jnp.where(other == 0, cx // 2, 1 - cx // 2)
        g, h, _ = parts[0]
        lax.fori_loop(at, upto, pump, 0)

        for n, name in ((1, FULL), (2, FULL2), (3, FULL3)):
            @pl.when(op == name)
            def _():
                full(parts[:n])

        @pl.when(op == DIAG)
        def _():
            lower = jnp.where(half == 0, y == 1, y == 0)

            @pl.when(extra)
            def _():
                diag(8, 1, 7, (True, True, False, False), False)

            @pl.when(jnp.logical_not(extra))
            def _():
                @pl.when(other == 0)
                def _():
                    q_both(h, half, 1).wait_recv()

                @pl.when(other == 1)
                def _():
                    q_both(h, half, 2).wait_recv()
                    q_both(h, half, 3).wait_recv()

                @pl.when(lower)
                def _():
                    diag(g, h, b, (True,) * 4, True)

                @pl.when(jnp.logical_not(lower))
                def _():
                    diag(g, h, b, (False,) * 4, True)

        @pl.when(op == FIN)
        def _():
            def finish(tile):
                ob[tile] = (ab[tile] / jnp.sum(lb[tile], axis=1, keepdims=True)).astype(jnp.bfloat16)

            @pl.when(extra)
            def _():
                for far, targets in ((1 - cx // 2, (2, 3)), (cx // 2, (1, 0))):
                    for t in BOTH:
                        finish(32 + 2 * far + t)
                    for d in targets:
                        xo_send(d).start()

            @pl.when(jnp.logical_not(extra))
            def _():
                for t in range(4):
                    finish(g * 4 + t)

                @pl.when(other == 0)
                def _():
                    o_send(h, half, 1).start()
                    o_own(h, half).start()

                @pl.when(other == 1)
                def _():
                    o_send(h, half, 2).start()
                    o_send(h, half, 3).start()

        @pl.when(op == OTHER)
        def _():
            @pl.when(b == 0)
            def _():
                relay_own(1)

            @pl.when(b == 1)
            def _():
                for d in OTHERS:
                    q_both(1, 1, d).wait_recv()
                for n in (1,):
                    x_send(n)

            @pl.when(b == 2)
            def _():
                for d in range(4):
                    z_own(1, 1, d, 0)

                @pl.when(first)
                def _():
                    x_send(0)

            @pl.when(b == 3)
            def _():
                x_both(0).wait_recv()

        return upto

    lax.fori_loop(0, pick(z, STEPS), run, jnp.int32(0))

    lax.fori_loop(0, pick(z, TAKEN), fwd_wait, 0)

    def z_wait(h, half, d, way):
        z_piece(h, half, d, way).wait_send()

    for h in BOTH:
        for half in BOTH:
            for d in OTHERS:
                kv_both(h, half, d).wait_send()
                q_send(h, half, d).wait_send()
            for d in range(4):
                z_each(h, half, d, z_wait)
                if (h, half) == (1, 1):
                    @pl.when(z < 2)
                    def _():
                        z_wait(h, half, d, 0)

            def o_wait():
                o_own(h, half).wait()
                for d in OTHERS:
                    o_send(h, half, d).wait_send()
                    o_recv(h, half, d).wait_recv()

            if (h, half) == (1, 1):
                pl.when(jnp.logical_not(first))(o_wait)
            else:
                o_wait()

    @pl.when(first)
    def _():
        for n in BOTH:
            x_both(n).wait_send()
            for d in range(4):
                xo_recv(n, d).wait_recv()

    @pl.when(has_x)
    def _():
        for d in range(4):
            xo_send(d).wait_send()


PARTS = 8


def by_rows(x_ref, o_ref, x_in, out, in_sem, out_sem):
    rows = 256 // PARTS

    def fetch(n):
        at = pl.ds(n * rows, rows)
        return pltpu.make_async_copy(x_ref.at[:, at], x_in.at[n], in_sem.at[n])

    def put(n):
        at = pl.ds(n * rows, rows)
        return pltpu.make_async_copy(out.at[at], o_ref.at[at], out_sem.at[n])

    for n in range(PARTS):
        fetch(n).start()
    for n in range(PARTS):
        fetch(n).wait()
        for g in range(4):
            out[n * rows:(n + 1) * rows, 8 * g:8 * g + 8] = jnp.swapaxes(x_in[n, 8 * g:8 * g + 8], 0, 1)
        put(n).start()
    for n in range(PARTS):
        put(n).wait()


def solution(mesh):
    spec = P(("dp", "cy", "cx"))

    def local(q, k, v):
        dma = pltpu.SemaphoreType.DMA
        out = pl.pallas_call(
            kernel,
            out_shape=jax.ShapeDtypeStruct((32, 256, HD), jnp.bfloat16),
            in_specs=[pl.BlockSpec(memory_space=pl.ANY)] * 3,
            out_specs=pl.BlockSpec(memory_space=pl.ANY),
            scratch_shapes=[
                pltpu.VMEM((256, 32, HD), jnp.bfloat16),
                pltpu.VMEM((256, 8, HD), jnp.bfloat16),
                pltpu.VMEM((256, 8, HD), jnp.bfloat16),
                pltpu.VMEM((32, 256, HD), jnp.bfloat16),
                pltpu.VMEM((8, 256, HD), jnp.bfloat16),
                pltpu.VMEM((8, 256, HD), jnp.bfloat16),
                pltpu.VMEM((36, 256, HD), jnp.bfloat16),
                pltpu.VMEM((2, 8, 2, B, HD), jnp.bfloat16),
                pltpu.VMEM((36, 256, HD), jnp.bfloat16),
                pltpu.VMEM((36, 256, HD), jnp.float32),
                pltpu.VMEM((36, 256, HD), jnp.float32),
                pltpu.VMEM((36, 256, HD), jnp.float32),
                dma((2, 2, 3)), dma((2, 2, 3)),
                dma((2, 2, 3)), dma((2, 2, 3)),
                dma((2, 2, 4, 2)), dma((2, 8)), dma((2, 8)),
                dma((2, 2, 3)), dma((2, 2, 3)),
                dma((2,)), dma((1,)), dma((4,)), dma((2, 4)),
                dma((3,)), dma((2, 2)),
            ],
            compiler_params=pltpu.CompilerParams(
                collective_id=0, has_side_effects=True, vmem_limit_bytes=60 * 1024 * 1024),
        )(q, k, v)
        return pl.pallas_call(
            by_rows,
            out_shape=jax.ShapeDtypeStruct((256, 32, HD), jnp.bfloat16),
            in_specs=[pl.BlockSpec(memory_space=pl.ANY)],
            out_specs=pl.BlockSpec(memory_space=pl.ANY),
            scratch_shapes=[
                pltpu.VMEM((PARTS, 32, 256 // PARTS, HD), jnp.bfloat16),
                pltpu.VMEM((256, 32, HD), jnp.bfloat16),
                dma((PARTS,)), dma((PARTS,)),
            ],
            compiler_params=pltpu.CompilerParams(vmem_limit_bytes=60 * 1024 * 1024),
        )(out)

    return jax.shard_map(local, mesh=mesh, in_specs=(spec, spec, spec), out_specs=spec, check_vma=False)
```
